256 devices in a mesh: gx: 8 (over z), gy: 4 (over y), gz: 8 (over x, core).
Axes of the slice: x: 4, y: 4, z: 8, core: 2. Of those that a mesh axis runs over, the one named last changes fastest.
Arguments:
- schur: bfloat16 [8, 4, 8, 2048, 2048], P('gx', 'gy', 'gz'), may hold values from -0.09375 to 0.09375
- interface_diag: float32 [8, 4, 8, 2048], P('gx', 'gy', 'gz'), may hold values from 2 to 4
- precond: float32 [8, 4, 8, 16, 128, 128], P('gx', 'gy', 'gz'), may hold values from -0.3 to 0.8
- load: bfloat16 [8, 4, 8, 2048, 256], P('gx', 'gy', 'gz'), may hold values from -170 to 170
- face_blocks: int32 [8, 4, 8, 6, 2], P('gx', 'gy', 'gz'), may hold values from 0 to 16, as said below
Outputs:
- solution: float32 [8, 4, 8, 2048, 256], P('gx', 'gy', 'gz')
- residual_norm: float32 [256], replicated
The draws below stay inside these ranges and needn't reach their ends.
Inputs may be any that keep to these rules, and one draw needn't show every extreme that they name: `face_blocks`: for each subdomain p and direction d (0, 1: next and previous along the first grid dimension; 2, 3 and 4, 5 likewise along the second and third), slots 0 to n - 1 hold block numbers below 16 shared with the neighbour in that direction, where n (1 to 2 inside the grid, 0 across its boundary) equals the neighbour's n for the opposite direction, and the neighbour's slot k of the opposite direction holds the block that shares with p's slot k; the remaining slots hold 16; no block number appears twice in one subdomain's table; some face shares 2 blocks in every draw.
All inputs are finite; a program needn't handle non-finite values.
Results may differ from the reference program's by a relative error of at most 0.0008.
Values sent between devices are 32-bit elements; how exact they have to be, the bound alone decides.
No kernel may reach another device: no remote copies, remote signals or barrier semaphores. Data moves between devices by JAX's collectives and lax.ppermute only.
A program may use at most 128 MiB of HBM per device.

```python
import math
import jax
import jax.numpy as jnp
from jax import lax

BLK = 128
NBLK = 16
IFACE = 2048
CAP = 2
NRHS = 256
SUB_X = 8
SUB_Y = 4
SUB_Z = 8


def draw_precond(key, part):
    full_shape = (SUB_X, SUB_Y, SUB_Z, NBLK, BLK, BLK)
    key_diag, key_off = jax.random.split(jax.random.fold_in(key, 11))
    diagonal = 1.0 / jax.random.uniform(key_diag, full_shape[:-1], jnp.float32, 2.0, 4.0)
    coupling = jnp.clip(jax.random.normal(key_off, full_shape, jnp.float32), -6.0, 6.0) * (0.12 / math.sqrt(BLK))
    identity = jnp.eye(BLK, dtype=jnp.float32)
    return coupling + diagonal[..., None] * identity


def ramp_factor(length):
    return jnp.power(3.0, jnp.arange(length, dtype=jnp.float32) / max(length - 1, 1))


def draw_load(key, part):
    key_base = jax.random.fold_in(jax.random.fold_in(key, 5), 0)
    key_rows = jax.random.fold_in(jax.random.fold_in(key, 5), 2)
    key_cols = jax.random.fold_in(jax.random.fold_in(key, 5), 3)
    full_shape = (SUB_X, SUB_Y, SUB_Z, NBLK * BLK, NRHS)
    row_scale = jnp.exp(jax.random.uniform(key_rows, full_shape[:4] + (1,), jnp.float32, 0.0, math.log(10.0)))
    col_scale = jnp.exp(jax.random.uniform(key_cols, (NRHS,), jnp.float32, 0.0, math.log(10.0)))
    position = ramp_factor(SUB_X)[:, None, None] * ramp_factor(SUB_Y)[None, :, None] * ramp_factor(SUB_Z)[None, None, :]
    base = jnp.clip(jax.random.normal(key_base, full_shape, jnp.float32), -6.0, 6.0)
    values = 0.01 * base * row_scale * col_scale * position[..., None, None]
    return values.astype(jnp.bfloat16)


def pair_counts(pair_key, axis_id):
    grid_shape = [SUB_X, SUB_Y, SUB_Z]
    grid_shape[axis_id] = grid_shape[axis_id] - 1
    counts = jax.random.randint(pair_key, tuple(grid_shape), 1, CAP + 1, dtype=jnp.int32)
    if grid_shape[axis_id] > 0:
        counts = counts.at[0, 0, 0].set(CAP)
    pad_upper = [(0, 0)] * 3
    pad_upper[axis_id] = (0, 1)
    pad_lower = [(0, 0)] * 3
    pad_lower[axis_id] = (1, 0)
    return (jnp.pad(counts, pad_upper), jnp.pad(counts, pad_lower))


def draw_face_blocks(key, part):
    key_x, key_y, key_z, key_perm = jax.random.split(jax.random.fold_in(key, 7), 4)
    upper_x, lower_x = pair_counts(key_x, 0)
    upper_y, lower_y = pair_counts(key_y, 1)
    upper_z, lower_z = pair_counts(key_z, 2)
    dir_counts = jnp.stack([upper_x, lower_x, upper_y, lower_y, upper_z, lower_z], axis=-1)
    offsets = jnp.cumsum(dir_counts, axis=-1) - dir_counts
    subdomains = SUB_X * SUB_Y * SUB_Z
    perm_keys = jax.random.split(key_perm, subdomains)
    orders = jax.vmap(lambda one_key: jax.random.permutation(one_key, NBLK))(perm_keys).astype(jnp.int32)
    orders = orders.reshape(SUB_X, SUB_Y, SUB_Z, 1, NBLK)
    slot_ids = jnp.arange(CAP, dtype=jnp.int32)
    positions = jnp.minimum(offsets[..., None] + slot_ids, NBLK - 1).astype(jnp.int32)
    picked = jnp.take_along_axis(orders, positions.reshape(SUB_X, SUB_Y, SUB_Z, 1, 6 * CAP), axis=-1)
    picked = picked.reshape(SUB_X, SUB_Y, SUB_Z, 6, CAP)
    valid = slot_ids < dir_counts[..., None]
    return jnp.where(valid, picked, NBLK).astype(jnp.int32)


def block_levels(own_key, shape, pieces, least, top_value):
    gain = 1.0
    for dim, parts in pieces:
        draws = jax.random.uniform(jax.random.fold_in(jax.random.fold_in(own_key, 6), dim), (parts,), jnp.float32, least / len(pieces), top_value / len(pieces))
        gain = gain * jnp.repeat(jnp.exp(draws), shape[dim] // parts).reshape((-1,) + (1,) * (len(shape) - 1 - dim))
    return gain


def gaussian(stream_key, shape, width, reach, shards=(), kind=jnp.bfloat16):
    result = width * jax.random.normal(stream_key, shape, jnp.float32)
    if shards:
        result = result * block_levels(stream_key, shape, shards, -0.22, 0.18)
    return jnp.clip(result, -reach, reach).astype(kind)


def setup_inputs(seed: int = 0) -> dict:
    seeds = jax.random.split(jax.random.key(seed), 6)
    return {
        "schur": gaussian(seeds[0], (SUB_X, SUB_Y, SUB_Z, IFACE, IFACE), (2 * IFACE) ** -0.5, 0.09375, ((0, 8), (1, 4), (2, 8))),
        "interface_diag": jnp.clip(jnp.exp(math.log(4.0) - 0.6931472 * jax.random.uniform(seeds[1], (SUB_X, SUB_Y, SUB_Z, IFACE), jnp.float32) ** block_levels(seeds[1], (SUB_X, SUB_Y, SUB_Z, IFACE), ((0, 8), (1, 4), (2, 8)), -0.2, 0.2)), 2.0, 4.0),
        "precond": draw_precond(jax.random.fold_in(seeds[5], 71), 0),
        "load": draw_load(jax.random.fold_in(seeds[5], 71), 0),
        "face_blocks": draw_face_blocks(jax.random.fold_in(seeds[5], 71), 0),
    }


epsilon = 1e-06

def find_live(face_blocks):
    slot_hits = face_blocks[..., None] == jnp.arange(NBLK, dtype=jnp.int32)
    return jnp.any(slot_hits, axis=(3, 4)).astype(jnp.float32)

def from_next(values, axis_id):
    length = values.shape[axis_id]
    pad_spec = [(0, 0)] * values.ndim
    pad_spec[axis_id] = (0, 1)
    return lax.slice_in_dim(jnp.pad(values, pad_spec), 1, length + 1, axis=axis_id)

def from_prev(values, axis_id):
    length = values.shape[axis_id]
    pad_spec = [(0, 0)] * values.ndim
    pad_spec[axis_id] = (1, 0)
    return lax.slice_in_dim(jnp.pad(values, pad_spec), 0, length, axis=axis_id)

def assemble(blocks, face_blocks, live_mask):
    grid_shape = blocks.shape[:3]
    row_width = blocks.shape[-1]
    subdomains = grid_shape[0] * grid_shape[1] * grid_shape[2]
    flattened = blocks.reshape(subdomains, NBLK, BLK, row_width)
    extended = jnp.concatenate([flattened, jnp.zeros((subdomains, 1, BLK, row_width), jnp.float32)], axis=1)
    slot_index = face_blocks.reshape(subdomains, 6 * CAP).astype(jnp.int32)
    packed = jax.vmap(lambda table, picks: table[picks])(extended, slot_index)
    packed = packed.reshape(grid_shape + (6, CAP, BLK, row_width))
    arrived = jnp.stack([from_next(packed[:, :, :, 1], 0), from_prev(packed[:, :, :, 0], 0), from_next(packed[:, :, :, 3], 1), from_prev(packed[:, :, :, 2], 1), from_next(packed[:, :, :, 5], 2), from_prev(packed[:, :, :, 4], 2)], axis=3)
    arrived = arrived.reshape(subdomains, 6 * CAP, BLK, row_width)
    extended = jax.vmap(lambda table, picks, extra: table.at[picks].add(extra))(extended, slot_index, arrived)
    return extended[:, :NBLK].reshape(blocks.shape) * live_mask[..., None, None]

def inner_product(left_vec, right_vec):
    return 0.5 * lax.optimization_barrier(jnp.sum(left_vec * right_vec, axis=(0, 1, 2, 3, 4)))

def precondition(vector, precond, face_blocks, live_mask):
    partial_value = jnp.einsum('xyzbij,xyzbjr->xyzbir', precond, vector, precision=lax.Precision.HIGHEST)
    return assemble(partial_value, face_blocks, live_mask)

def operate(vector, schur, interface_diag, face_blocks, live_mask):
    subdomains = SUB_X * SUB_Y * SUB_Z
    flat_schur = schur.reshape(subdomains, IFACE, IFACE)
    flat_vector = vector.reshape(subdomains, IFACE, NRHS)
    product = lax.map(lambda pair: jnp.dot(pair[0], pair[1].astype(jnp.bfloat16), preferred_element_type=jnp.float32), (flat_schur, flat_vector))
    partial_value = product + interface_diag.reshape(subdomains, IFACE, 1) * flat_vector
    return assemble(partial_value.reshape(vector.shape), face_blocks, live_mask)

def reference(schur, interface_diag, precond, load, face_blocks):
    live_mask = find_live(face_blocks)
    block_shape = (SUB_X, SUB_Y, SUB_Z, NBLK, BLK, NRHS)
    assembled_load = assemble(load.astype(jnp.float32).reshape(block_shape), face_blocks, live_mask)
    initial = jnp.sqrt(inner_product(assembled_load, assembled_load) + epsilon)
    basis_first = assembled_load / initial
    precond_first = precondition(basis_first, precond, face_blocks, live_mask)
    working = operate(precond_first, schur, interface_diag, face_blocks, live_mask)
    diag_first = inner_product(working, basis_first)
    working = working - diag_first * basis_first
    below_first = jnp.sqrt(inner_product(working, working) + epsilon)
    basis_second = working / below_first
    precond_second = precondition(basis_second, precond, face_blocks, live_mask)
    working = operate(precond_second, schur, interface_diag, face_blocks, live_mask)
    upper_second = inner_product(working, basis_first)
    working = working - upper_second * basis_first
    diag_second = inner_product(working, basis_second)
    working = working - diag_second * basis_second
    below_second = jnp.sqrt(inner_product(working, working) + epsilon)
    radius_first = jnp.sqrt(diag_first * diag_first + below_first * below_first)
    cosine_first = diag_first / radius_first
    sine_first = below_first / radius_first
    rotated_top = cosine_first * upper_second + sine_first * diag_second
    rotated_low = cosine_first * diag_second - sine_first * upper_second
    radius_second = jnp.sqrt(rotated_low * rotated_low + below_second * below_second)
    cosine_second = rotated_low / radius_second
    sine_second = below_second / radius_second
    weight_second = -initial * sine_first * cosine_second / radius_second
    weight_first = (initial * cosine_first - rotated_top * weight_second) / radius_first
    solution = weight_first * precond_first + weight_second * precond_second
    residual_norm = initial * sine_first * sine_second
    return (solution.reshape(SUB_X, SUB_Y, SUB_Z, IFACE, NRHS), residual_norm)
```

```python
import jax
import jax.numpy as jnp
from jax import lax
from jax.experimental import pallas as pl
from jax.experimental.pallas import tpu as pltpu
from jax.sharding import Mesh
from jax.sharding import PartitionSpec as P

GZ = ("gz_0", "gz_1")
INNER = ("gy", "gz_0", "gz_1")

epsilon = 1e-06
F32 = jnp.float32
BF16 = jnp.bfloat16
VMEM_MIB = 28


def call(body, outs, operands, scratch=(), smem=1, raw=()):
    specs = []
    operands = list(operands)
    for i in range(len(operands)):
        if i < smem:
            specs.append(pl.BlockSpec(memory_space=pltpu.SMEM))
        elif i in raw:
            specs.append(pl.BlockSpec(memory_space=pltpu.HBM))
            operands[i] = pltpu.with_memory_space_constraint(operands[i], pltpu.HBM)
        else:
            specs.append(pl.BlockSpec(memory_space=pltpu.VMEM))
    return pl.pallas_call(
        body,
        out_shape=[jax.ShapeDtypeStruct(s, t) for s, t in outs],
        in_specs=specs,
        out_specs=[pl.BlockSpec(memory_space=pltpu.VMEM) for _ in outs],
        scratch_shapes=list(scratch),
        compiler_params=pltpu.CompilerParams(vmem_limit_bytes=VMEM_MIB * 2**20),
    )(*operands)


def shifts(axis):
    n = lax.axis_size(axis)
    up = [(i, (i + 1) % n) for i in range(n)]
    return up, [(j, i) for i, j in up]


def exchange(faces):
    got = [None] * 6
    for a, axis in enumerate(("gx", "gy", GZ)):
        up, down = shifts(axis)
        got[2 * a] = lax.ppermute(faces[2 * a + 1], axis, down)
        got[2 * a + 1] = lax.ppermute(faces[2 * a], axis, up)
    return got


def exchange_once(messages):
    got = []
    for message, axis in zip(messages, ("gx", "gy")):
        n = lax.axis_size(axis)
        pairs = []
        for i in range(n):
            pairs += [(2 * i, 2 * ((i + 1) % n)), (2 * i + 1, 2 * ((i - 1) % n) + 1)]
        got.append(lax.ppermute(message, (axis, "gz_1"), pairs))
    got.append(lax.ppermute(messages[2], GZ, shifts(GZ)[0]))
    return got


def gather_sum(rows, axes):
    n = lax.axis_size(axes)
    wide = jnp.broadcast_to(rows[None], (n,) + rows.shape).reshape(n * rows.shape[0], rows.shape[1])
    wide = lax.all_to_all(wide, axes, 0, 0, tiled=True)
    return jnp.sum(wide.reshape((n,) + rows.shape), axis=0)


def total(rows):
    return gather_sum(gather_sum(rows, INNER), ("gx",))


def split(x):
    hi = x.astype(BF16)
    return hi, (x - hi.astype(F32)).astype(BF16)


def apply_block(mcat, vec):
    blk = mcat.shape[0]
    hi, lo = split(vec)
    out = jnp.dot(mcat, jnp.concatenate([hi, hi], axis=0), preferred_element_type=F32)
    return out + jnp.dot(mcat[:, :blk], lo, preferred_element_type=F32)


def column(row, blk):
    r = lax.broadcasted_iota(jnp.int32, (blk, blk), 0)
    c = lax.broadcasted_iota(jnp.int32, (blk, blk), 1)
    return jnp.sum(jnp.where(r == c, jnp.broadcast_to(row, (blk, blk)), 0.0), axis=1, keepdims=True)


def colsum(x):
    return jnp.sum(x, axis=0, keepdims=True)


def on_device(schur, interface_diag, precond, load, face_blocks):
    nblk, blk = precond.shape[3], precond.shape[4]
    cols = load.shape[-1]
    order = nblk * blk
    cap = face_blocks.shape[-1]
    slots = 6 * cap
    rows = cap * blk
    table = face_blocks.reshape(slots)
    core = lax.axis_index("gz_1").reshape(1).astype(jnp.int32)
    matrix = schur.reshape(order, order)
    diag = interface_diag.reshape(nblk, blk)

    def pick(table_ref, i):
        b = table_ref[i]
        return jnp.minimum(b, nblk - 1), (b < nblk).astype(F32), b

    def pack(table_ref, load_ref, pre_ref, *faces):
        for i in range(slots):
            b, m, _ = pick(table_ref, i)
            d, at = i // cap, (i % cap) * blk
            faces[d][at : at + blk, :cols] = load_ref[pl.ds(b * blk, blk), :].astype(F32) * m
            faces[d][at : at + blk, cols:] = pre_ref[b] * m

    faces = call(
        pack,
        [((rows, cols + blk), F32)] * 6,
        (table, load.reshape(order, cols), precond.reshape(nblk, blk, blk)),
    )
    came = exchange(faces)

    def spread(table_ref, zb_ref, i, value):
        b = table_ref[i]

        @pl.when(b < nblk)
        def _():
            zb_ref[pl.ds(pl.multiple_of(b * blk, blk), blk), :] = value.astype(BF16)

    def local_schur(table_ref, d, s_tile, zb_ref, z_ref, diag_ref):
        product = jnp.dot(s_tile, zb_ref[...], preferred_element_type=F32)
        parts = []
        for k in range(cap):
            i = d * cap + k
            b, m, _ = pick(table_ref, i)
            z = z_ref[i * blk : (i + 1) * blk, :]
            dcol = column(diag_ref[pl.ds(b, 1), :], blk)
            parts.append((product[k * blk : (k + 1) * blk] + dcol * z) * m)
        return parts

    def fetch(table_ref, matrix_ref, s_ref, sems):
        copies = []
        for i in range(slots):
            b, _, _ = pick(table_ref, i)
            copy = pltpu.make_async_copy(
                matrix_ref.at[pl.ds(pl.multiple_of(b * blk, blk), blk), :],
                s_ref.at[pl.ds(i * blk, blk), :],
                sems.at[i],
            )
            copy.start()
            copies.append(copy)
        return copies

    def first(table_ref, *refs):
        own, got = refs[:6], refs[6:12]
        diag_ref, matrix_ref = refs[12], refs[13]
        r_ref, z_ref, m_ref, sum_ref = refs[14:18]
        y_refs = refs[18:24]
        zb_ref, s_ref, sems = refs[24:27]
        copies = fetch(table_ref, matrix_ref, s_ref, sems)
        zb_ref[...] = jnp.zeros_like(zb_ref)
        square = jnp.zeros((1, cols), F32)
        for i in range(slots):
            d, at = i // cap, (i % cap) * blk
            r = own[d][at : at + blk, :cols] + got[d][at : at + blk, :cols]
            m = own[d][at : at + blk, cols:] + got[d][at : at + blk, cols:]
            hi, lo = split(m)
            mcat = jnp.concatenate([hi, lo], axis=1)
            m_ref[i * blk : (i + 1) * blk, :] = mcat
            r_ref[i * blk : (i + 1) * blk, :] = r
            square += colsum(r * r)
            z = apply_block(mcat, r)
            z_ref[i * blk : (i + 1) * blk, :] = z
            spread(table_ref, zb_ref, i, z)
        cross = jnp.zeros((1, cols), F32)
        for d in range(6):
            for k in range(cap):
                copies[d * cap + k].wait()
            parts = local_schur(
                table_ref, d, s_ref[d * rows : (d + 1) * rows, :], zb_ref, z_ref, diag_ref
            )
            for k in range(cap):
                i = d * cap + k
                y_refs[d][k * blk : (k + 1) * blk, :] = parts[k]
                cross += colsum(parts[k] * r_ref[i * blk : (i + 1) * blk, :])
        sum_ref[...] = jnp.zeros_like(sum_ref)
        sum_ref[0:1, :] = 0.5 * square
        sum_ref[1:2, :] = cross

    scratch = (
        pltpu.VMEM((order, cols), BF16),
        pltpu.VMEM((slots * blk, order), BF16),
        pltpu.SemaphoreType.DMA((slots,)),
    )
    r, z1, mcat, sums, *ys = call(
        first,
        [
            ((slots * blk, cols), F32),
            ((slots * blk, cols), F32),
            ((slots * blk, 2 * blk), BF16),
            ((8, cols), F32),
        ]
        + [((rows, cols), F32)] * 6,
        (table, *faces, *came, diag, matrix),
        scratch=scratch,
        raw=(14,),
    )
    came = exchange(ys)
    first_sums = total(sums)

    def second(table_ref, core_ref, *refs):
        own, got = refs[:6], refs[6:12]
        r_ref, m_ref, diag_ref, red_ref, matrix_ref = refs[12:17]
        z_ref, sum_ref = refs[17:19]
        y_refs, msgs = refs[19:25], refs[25:28]
        zb_ref, s_ref, sems, w_ref = refs[28:32]
        copies = fetch(table_ref, matrix_ref, s_ref, sems)
        inv = 1.0 / jnp.sqrt(red_ref[0:1, :] + epsilon)
        h11 = red_ref[1:2, :] * inv * inv
        zb_ref[...] = jnp.zeros_like(zb_ref)
        square = jnp.zeros((1, cols), F32)
        for i in range(slots):
            d, at = i // cap, (i % cap) * blk
            w = own[d][at : at + blk, :] + got[d][at : at + blk, :]
            w = (w - h11 * r_ref[i * blk : (i + 1) * blk, :]) * inv
            w_ref[i * blk : (i + 1) * blk, :] = w
            square += colsum(w * w)
            z = apply_block(m_ref[i * blk : (i + 1) * blk, :], w)
            z_ref[i * blk : (i + 1) * blk, :] = z
            spread(table_ref, zb_ref, i, z)
        on_first = jnp.zeros((1, cols), F32)
        on_second = jnp.zeros((1, cols), F32)
        low = core_ref[0] == 0
        for d in range(6):
            for k in range(cap):
                copies[d * cap + k].wait()
            parts = local_schur(
                table_ref, d, s_ref[d * rows : (d + 1) * rows, :], zb_ref, z_ref, diag_ref
            )
            for k in range(cap):
                i = d * cap + k
                y_refs[d][k * blk : (k + 1) * blk, :] = parts[k]
                on_first += colsum(parts[k] * r_ref[i * blk : (i + 1) * blk, :])
                on_second += colsum(parts[k] * w_ref[i * blk : (i + 1) * blk, :])
        for a in range(2):

            @pl.when(low)
            def _():
                msgs[a][...] = y_refs[2 * a][...]

            @pl.when(jnp.logical_not(low))
            def _():
                msgs[a][...] = y_refs[2 * a + 1][...]

        msgs[2][...] = y_refs[4][...]
        sum_ref[...] = jnp.zeros_like(sum_ref)
        sum_ref[0:1, :] = 0.5 * square
        sum_ref[1:2, :] = on_first * inv
        sum_ref[2:3, :] = on_second

    z2, sums, *rest = call(
        second,
        [((slots * blk, cols), F32), ((8, cols), F32)] + [((rows, cols), F32)] * 9,
        (table, core, *ys, *came, r, mcat, diag, first_sums, matrix),
        scratch=scratch + (pltpu.VMEM((slots * blk, cols), F32),),
        smem=2,
        raw=(18,),
    )
    ys, msgs = rest[:6], rest[6:]
    came = exchange_once(msgs)

    def norms(core_ref, *refs):
        own, got, in_ref, out_ref, acc_ref = refs[:6], refs[6:9], refs[9], refs[10], refs[11]
        low = core_ref[0] == 0
        out_ref[...] = in_ref[...]
        both = own[5][...] + got[2][...]
        acc_ref[...] = colsum(both * both)
        for a in range(2):

            @pl.when(low)
            def _():
                both = own[2 * a + 1][...] + got[a][...]
                acc_ref[...] += colsum(both * both)

            @pl.when(jnp.logical_not(low))
            def _():
                both = own[2 * a][...] + got[a][...]
                acc_ref[...] += colsum(both * both)

        out_ref[3:4, :] = acc_ref[...]

    (sums,) = call(
        norms,
        [((8, cols), F32)],
        (core, *ys, *came, sums),
        scratch=(pltpu.VMEM((1, cols), F32),),
    )
    second_sums = total(sums)

    def finish(table_ref, z1_ref, z2_ref, one_ref, two_ref, out_ref, res_ref):
        load_square = one_ref[0:1, :]
        initial = jnp.sqrt(load_square + epsilon)
        rescale = 1.0 / initial
        h11 = one_ref[1:2, :] * rescale * rescale
        w_square = two_ref[0:1, :]
        h21 = jnp.sqrt(w_square + epsilon)
        down = 1.0 / h21
        h12 = two_ref[1:2, :] * down
        dot22 = two_ref[2:3, :] * down * down
        square = two_ref[3:4, :] * down * down
        g11 = load_square * rescale * rescale
        g22 = w_square * down * down
        g12 = h11 * (epsilon * rescale * rescale) * down
        h22 = dot22 - h12 * g12
        left = square - h12 * h12 * (2.0 - g11) - h22 * (2.0 * dot22 - h22 * g22) + 2.0 * h12 * h22 * g12
        h32 = jnp.sqrt(jnp.maximum(left, 0.0) + epsilon)
        r1 = jnp.sqrt(h11 * h11 + h21 * h21)
        c1, s1 = h11 / r1, h21 / r1
        top = c1 * h12 + s1 * h22
        bottom = c1 * h22 - s1 * h12
        r2 = jnp.sqrt(bottom * bottom + h32 * h32)
        c2, s2 = bottom / r2, h32 / r2
        y2 = -initial * s1 * c2 / r2
        y1 = (initial * c1 - top * y2) / r1
        res_ref[...] = initial * s1 * s2
        a1 = y1 * rescale
        a2 = y2 * down
        out_ref[...] = jnp.zeros_like(out_ref)
        for i in range(slots):
            b = table_ref[i]

            @pl.when(b < nblk)
            def _():
                z = a1 * z1_ref[i * blk : (i + 1) * blk, :] + a2 * z2_ref[i * blk : (i + 1) * blk, :]
                out_ref[pl.ds(pl.multiple_of(b * blk, blk), blk), :] = z

    out, res = call(
        finish,
        [((order, cols), F32), ((1, cols), F32)],
        (table, z1, z2, first_sums, second_sums),
    )
    return out.reshape(1, 1, 1, order, cols), res.reshape(cols)


def solution(mesh):
    torus = Mesh(
        mesh.devices.reshape(mesh.shape["gx"], mesh.shape["gy"], 4, 2), ("gx", "gy", "gz_0", "gz_1")
    )
    in_specs = (
        P("gx", "gy", GZ, None, None),
        P("gx", "gy", GZ, None),
        P("gx", "gy", GZ, None, None, None),
        P("gx", "gy", GZ, None, None),
        P("gx", "gy", GZ, None, None),
    )
    out_specs = (P("gx", "gy", GZ, None, None), P())
    return jax.shard_map(
        on_device, mesh=torus, in_specs=in_specs, out_specs=out_specs, check_vma=False
    )
```

```python
import jax
import jax.numpy as jnp
from jax import lax
from jax.experimental import pallas as pl
from jax.experimental.pallas import tpu as pltpu
from jax.sharding import Mesh
from jax.sharding import PartitionSpec as P

GZ = ("gz_0", "gz_1")
INNER = ("gy", "gz_0", "gz_1")

epsilon = 1e-06
F32 = jnp.float32
BF16 = jnp.bfloat16


def call(body, outs, operands, scratch=(), smem=1, raw=(), flops=0, mib=16):
    specs = []
    operands = list(operands)
    for i in range(len(operands)):
        if i < smem:
            specs.append(pl.BlockSpec(memory_space=pltpu.SMEM))
        elif i in raw:
            specs.append(pl.BlockSpec(memory_space=pltpu.HBM))
            operands[i] = pltpu.with_memory_space_constraint(operands[i], pltpu.HBM)
        else:
            specs.append(pl.BlockSpec(memory_space=pltpu.VMEM))
    return pl.pallas_call(
        body,
        out_shape=[jax.ShapeDtypeStruct(s, t) for s, t in outs],
        in_specs=specs,
        out_specs=[pl.BlockSpec(memory_space=pltpu.VMEM) for _ in outs],
        scratch_shapes=list(scratch),
        compiler_params=pltpu.CompilerParams(vmem_limit_bytes=mib * 2**20),
        cost_estimate=pl.CostEstimate(flops=flops, transcendentals=0, bytes_accessed=2**20),
    )(*operands)


def shifts(axis):
    n = lax.axis_size(axis)
    up = [(i, (i + 1) % n) for i in range(n)]
    return up, [(j, i) for i, j in up]


def exchange(faces):
    got = [None] * 6
    for a, axis in enumerate(("gx", "gy", GZ)):
        up, down = shifts(axis)
        got[2 * a] = lax.ppermute(faces[2 * a + 1], axis, down)
        got[2 * a + 1] = lax.ppermute(faces[2 * a], axis, up)
    return got


def exchange_once(messages):
    got = []
    for message, axis in zip(messages, ("gx", "gy")):
        n = lax.axis_size(axis)
        pairs = []
        for i in range(n):
            pairs += [(2 * i, 2 * ((i + 1) % n)), (2 * i + 1, 2 * ((i - 1) % n) + 1)]
        got.append(lax.ppermute(message, (axis, "gz_1"), pairs))
    got.append(lax.ppermute(messages[2], GZ, shifts(GZ)[0]))
    return got


def gather_sum(rows, axes):
    n = lax.axis_size(axes)
    wide = jnp.broadcast_to(rows[None], (n,) + rows.shape).reshape(n * rows.shape[0], rows.shape[1])
    wide = lax.all_to_all(wide, axes, 0, 0, tiled=True)
    return jnp.sum(wide.reshape((n,) + rows.shape), axis=0)


def total(rows):
    return gather_sum(gather_sum(rows, INNER), ("gx",))


def split(x):
    hi = x.astype(BF16)
    return hi, (x - hi.astype(F32)).astype(BF16)


def apply_block(mcat, vec):
    blk = mcat.shape[0]
    hi, lo = split(vec)
    out = jnp.dot(mcat, jnp.concatenate([hi, hi], axis=0), preferred_element_type=F32)
    return out + jnp.dot(mcat[:, :blk], lo, preferred_element_type=F32)


def column(row, blk):
    r = lax.broadcasted_iota(jnp.int32, (blk, blk), 0)
    c = lax.broadcasted_iota(jnp.int32, (blk, blk), 1)
    return jnp.sum(jnp.where(r == c, jnp.broadcast_to(row, (blk, blk)), 0.0), axis=1, keepdims=True)


def colsum(x):
    return jnp.sum(x, axis=0, keepdims=True)


def on_device(schur, interface_diag, precond, load, face_blocks):
    nblk, blk = precond.shape[3], precond.shape[4]
    cols = load.shape[-1]
    order = nblk * blk
    cap = face_blocks.shape[-1]
    slots = 6 * cap
    rows = cap * blk
    table = face_blocks.reshape(6, cap).T
    matrix = schur.reshape(order, order)
    diag = interface_diag.reshape(nblk, blk)

    def pick(table_ref, i):
        b = table_ref[i % cap, i // cap]
        return jnp.minimum(b, nblk - 1), (b < nblk).astype(F32)

    def pack(table_ref, load_ref, pre_ref, *refs):
        faces, (load_buf, pre_buf, load_sems, pre_sems) = refs[:6], refs[6:]
        copies = []
        for i in range(slots):
            b, _ = pick(table_ref, i)
            at = pl.multiple_of(b * blk, blk)
            copies.append(
                (
                    pltpu.make_async_copy(load_ref.at[pl.ds(at, blk), :], load_buf.at[i], load_sems.at[i]),
                    pltpu.make_async_copy(pre_ref.at[b], pre_buf.at[i], pre_sems.at[i]),
                )
            )
            for copy in copies[-1]:
                copy.start()
        for i in range(slots):
            _, m = pick(table_ref, i)
            d, at = i // cap, (i % cap) * blk
            for copy in copies[i]:
                copy.wait()
            faces[d][at : at + blk, :cols] = load_buf[i].astype(F32) * m
            faces[d][at : at + blk, cols:] = pre_buf[i] * m

    faces = call(
        pack,
        [((rows, cols + blk), F32)] * 6,
        (table, load.reshape(order, cols), precond.reshape(nblk, blk, blk)),
        scratch=(
            pltpu.VMEM((slots, blk, cols), BF16),
            pltpu.VMEM((slots, blk, blk), F32),
            pltpu.SemaphoreType.DMA((slots,)),
            pltpu.SemaphoreType.DMA((slots,)),
        ),
        raw=(1, 2),
    )
    came = exchange(faces)

    def fetch(table_ref, matrix_ref, s_ref, sems):
        copies = []
        for i in range(slots):
            b, _ = pick(table_ref, i)
            copy = pltpu.make_async_copy(
                matrix_ref.at[pl.ds(pl.multiple_of(b * blk, blk), blk), :],
                s_ref.at[pl.ds(i * blk, blk), :],
                sems.at[i],
            )
            copy.start()
            copies.append(copy)
        for copy in copies:
            copy.wait()

    (sel,) = call(
        fetch,
        [((slots * blk, order), BF16)],
        (table, matrix),
        scratch=(pltpu.SemaphoreType.DMA((slots,)),),
        raw=(1,),
        flops=2 * 10**9,
    )

    def spread(table_ref, zb_ref, i, value):
        b = table_ref[i % cap, i // cap]

        @pl.when(b < nblk)
        def _():
            zb_ref[pl.ds(pl.multiple_of(b * blk, blk), blk), :] = value.astype(BF16)

    def local_schur(table_ref, d, s_tile, zb_ref, z_ref, diag_ref):
        product = jnp.dot(s_tile, zb_ref[...], preferred_element_type=F32)
        parts = []
        for k in range(cap):
            i = d * cap + k
            b, m = pick(table_ref, i)
            z = z_ref[i * blk : (i + 1) * blk, :]
            dcol = column(diag_ref[pl.ds(b, 1), :], blk)
            parts.append((product[k * blk : (k + 1) * blk] + dcol * z) * m)
        return parts

    def first(table_ref, *refs):
        own, got = refs[:6], refs[6:12]
        diag_ref, s_ref = refs[12:14]
        r_ref, z_ref, m_ref, sum_ref = refs[14:18]
        y_refs = refs[18:24]
        zb_ref = refs[24]
        zb_ref[...] = jnp.zeros_like(zb_ref)
        square = jnp.zeros((1, cols), F32)
        for i in range(slots):
            d, at = i // cap, (i % cap) * blk
            r = own[d][at : at + blk, :cols] + got[d][at : at + blk, :cols]
            m = own[d][at : at + blk, cols:] + got[d][at : at + blk, cols:]
            hi, lo = split(m)
            mcat = jnp.concatenate([hi, lo], axis=1)
            m_ref[i * blk : (i + 1) * blk, :] = mcat
            r_ref[i * blk : (i + 1) * blk, :] = r
            square += colsum(r * r)
            z = apply_block(mcat, r)
            z_ref[i * blk : (i + 1) * blk, :] = z
            spread(table_ref, zb_ref, i, z)
        cross = jnp.zeros((1, cols), F32)
        for d in range(6):
            parts = local_schur(
                table_ref, d, s_ref[d * rows : (d + 1) * rows, :], zb_ref, z_ref, diag_ref
            )
            for k in range(cap):
                i = d * cap + k
                y_refs[d][k * blk : (k + 1) * blk, :] = parts[k]
                cross += colsum(parts[k] * r_ref[i * blk : (i + 1) * blk, :])
        sum_ref[...] = jnp.zeros_like(sum_ref)
        sum_ref[0:1, :] = 0.5 * square
        sum_ref[1:2, :] = cross

    spread_z = (pltpu.VMEM((order, cols), BF16),)
    long = slots * blk
    r, z1, mcat, sums, *ys = call(
        first,
        [((long, cols), F32), ((long, cols), F32), ((long, 2 * blk), BF16), ((8, cols), F32)]
        + [((rows, cols), F32)] * 6,
        (table, *faces, *came, diag, sel),
        scratch=spread_z,
        flops=2 * 10**9,
    )
    came = exchange(ys)

    def second(table_ref, *refs):
        own, got = refs[:6], refs[6:12]
        r_ref, m_ref, diag_ref, in_ref, s_ref = refs[12:17]
        z_ref, sum_ref = refs[17:19]
        y_refs, msgs = refs[19:25], refs[25:28]
        zb_ref, w_ref = refs[28:30]
        zb_ref[...] = jnp.zeros_like(zb_ref)
        square = jnp.zeros((1, cols), F32)
        for i in range(slots):
            d, at = i // cap, (i % cap) * blk
            w = own[d][at : at + blk, :] + got[d][at : at + blk, :]
            w_ref[i * blk : (i + 1) * blk, :] = w
            square += colsum(w * w)
            z = apply_block(m_ref[i * blk : (i + 1) * blk, :], w)
            z_ref[i * blk : (i + 1) * blk, :] = z
            spread(table_ref, zb_ref, i, z)
        on_first = jnp.zeros((1, cols), F32)
        on_second = jnp.zeros((1, cols), F32)
        low = lax.axis_index("gz_1") == 0
        for d in range(6):
            parts = local_schur(
                table_ref, d, s_ref[d * rows : (d + 1) * rows, :], zb_ref, z_ref, diag_ref
            )
            for k in range(cap):
                i = d * cap + k
                y_refs[d][k * blk : (k + 1) * blk, :] = parts[k]
                on_first += colsum(parts[k] * r_ref[i * blk : (i + 1) * blk, :])
                on_second += colsum(parts[k] * w_ref[i * blk : (i + 1) * blk, :])
        for a in range(2):

            @pl.when(low)
            def _():
                msgs[a][...] = y_refs[2 * a][...]

            @pl.when(jnp.logical_not(low))
            def _():
                msgs[a][...] = y_refs[2 * a + 1][...]

        msgs[2][...] = y_refs[4][...]
        sum_ref[...] = in_ref[...]
        sum_ref[2:3, :] = 0.5 * square
        sum_ref[3:4, :] = on_first
        sum_ref[4:5, :] = on_second

    z2, sums, *rest = call(
        second,
        [((long, cols), F32), ((8, cols), F32)] + [((rows, cols), F32)] * 9,
        (table, *ys, *came, r, mcat, diag, sums, sel),
        scratch=spread_z + (pltpu.VMEM((long, cols), F32),),
        flops=2 * 10**9,
    )
    ys, msgs = rest[:6], rest[6:]
    came = exchange_once(msgs)

    def norms(*refs):
        own, got, in_ref, out_ref, acc_ref = refs[:6], refs[6:9], refs[9], refs[10], refs[11]
        low = lax.axis_index("gz_1") == 0
        out_ref[...] = in_ref[...]
        both = own[5][...] + got[2][...]
        acc_ref[...] = colsum(both * both)
        for a in range(2):

            @pl.when(low)
            def _():
                both = own[2 * a + 1][...] + got[a][...]
                acc_ref[...] += colsum(both * both)

            @pl.when(jnp.logical_not(low))
            def _():
                both = own[2 * a][...] + got[a][...]
                acc_ref[...] += colsum(both * both)

        out_ref[5:6, :] = acc_ref[...]

    (sums,) = call(
        norms,
        [((8, cols), F32)],
        (*ys, *came, sums),
        scratch=(pltpu.VMEM((1, cols), F32),),
        smem=0,
    )
    sums = total(sums)

    def finish(table_ref, z1_ref, z2_ref, gram_ref, out_ref, res_ref):
        load_square = gram_ref[0:1, :]
        initial = jnp.sqrt(load_square + epsilon)
        rescale = 1.0 / initial
        scale2 = rescale * rescale
        h11 = gram_ref[1:2, :] * scale2
        b11 = gram_ref[2:3, :] * scale2
        c1v = gram_ref[3:4, :] * scale2
        c11 = gram_ref[4:5, :] * scale2
        e11 = gram_ref[5:6, :] * scale2
        g11 = load_square * scale2
        w_square = jnp.maximum(b11 - h11 * h11 * (2.0 - g11), 0.0)
        h21 = jnp.sqrt(w_square + epsilon)
        down = 1.0 / h21
        g22 = w_square * down * down
        g12 = h11 * (epsilon * scale2) * down
        h12 = (c1v - h11 * h11) * down
        dot22 = ((c11 - h11 * c1v) - h11 * (b11 - h11 * h11)) * down * down
        square = ((e11 - h11 * c11) - h11 * (c11 - h11 * b11)) * down * down
        h22 = dot22 - h12 * g12
        left = square - h12 * h12 * (2.0 - g11) - h22 * (2.0 * dot22 - h22 * g22) + 2.0 * h12 * h22 * g12
        h32 = jnp.sqrt(jnp.maximum(left, 0.0) + epsilon)
        r1 = jnp.sqrt(h11 * h11 + h21 * h21)
        c1, s1 = h11 / r1, h21 / r1
        top = c1 * h12 + s1 * h22
        bottom = c1 * h22 - s1 * h12
        r2 = jnp.sqrt(bottom * bottom + h32 * h32)
        c2, s2 = bottom / r2, h32 / r2
        y2 = -initial * s1 * c2 / r2
        y1 = (initial * c1 - top * y2) / r1
        res_ref[...] = initial * s1 * s2
        a2 = y2 * down * rescale
        a1 = y1 * rescale - a2 * h11
        out_ref[...] = jnp.zeros_like(out_ref)
        for i in range(slots):
            b = table_ref[i % cap, i // cap]

            @pl.when(b < nblk)
            def _():
                z = a1 * z1_ref[i * blk : (i + 1) * blk, :] + a2 * z2_ref[i * blk : (i + 1) * blk, :]
                out_ref[pl.ds(pl.multiple_of(b * blk, blk), blk), :] = z

    out, res = call(
        finish,
        [((order, cols), F32), ((1, cols), F32)],
        (table, z1, z2, sums),
    )
    return out.reshape(1, 1, 1, order, cols), res.reshape(cols)


def solution(mesh):
    torus = Mesh(
        mesh.devices.reshape(mesh.shape["gx"], mesh.shape["gy"], 4, 2), ("gx", "gy", "gz_0", "gz_1")
    )
    in_specs = (
        P("gx", "gy", GZ, None, None),
        P("gx", "gy", GZ, None),
        P("gx", "gy", GZ, None, None, None),
        P("gx", "gy", GZ, None, None),
        P("gx", "gy", GZ, None, None),
    )
    out_specs = (P("gx", "gy", GZ, None, None), P())
    return jax.shard_map(
        on_device, mesh=torus, in_specs=in_specs, out_specs=out_specs, check_vma=False
    )
```

```python
import jax
import jax.numpy as jnp
from jax import lax
from jax.experimental import pallas as pl
from jax.experimental.pallas import tpu as pltpu
from jax.sharding import Mesh
from jax.sharding import PartitionSpec as P

GZ = ("gz_0", "gz_1")
AXES = ("gx", "gy", GZ)
INNER = ("gy", "gz_0", "gz_1")


epsilon = 1e-06
F32 = jnp.float32
BF16 = jnp.bfloat16


def call(body, outs, operands, scratch=(), smem=1, raw=(), hbm_out=(), flops=0, mib=16):
    specs = []
    operands = list(operands)
    for i in range(len(operands)):
        if i < smem:
            specs.append(pl.BlockSpec(memory_space=pltpu.SMEM))
            operands[i] = pltpu.with_memory_space_constraint(operands[i], pltpu.HBM)
        elif i in raw:
            specs.append(pl.BlockSpec(memory_space=pltpu.HBM))
            operands[i] = pltpu.with_memory_space_constraint(operands[i], pltpu.HBM)
        else:
            specs.append(pl.BlockSpec(memory_space=pltpu.VMEM))
    return pl.pallas_call(
        body,
        out_shape=[jax.ShapeDtypeStruct(s, t) for s, t in outs],
        in_specs=specs,
        out_specs=[
            pl.BlockSpec(memory_space=pltpu.HBM if i in hbm_out else pltpu.VMEM) for i in range(len(outs))
        ],
        scratch_shapes=list(scratch),
        compiler_params=pltpu.CompilerParams(vmem_limit_bytes=mib * 2**20),
        cost_estimate=pl.CostEstimate(flops=flops, transcendentals=0, bytes_accessed=2**20),
    )(*operands)


def shifts(axis):
    n = lax.axis_size(axis)
    up = [(i, (i + 1) % n) for i in range(n)]
    return up, [(j, i) for i, j in up]


def exchange(to_next, to_previous, axis):
    up, down = shifts(axis)
    return [lax.ppermute(to_previous, axis, down), lax.ppermute(to_next, axis, up)]


def exchange_once(message, axis):
    if axis == GZ:
        return lax.ppermute(message, GZ, shifts(GZ)[0])
    n = lax.axis_size(axis)
    pairs = []
    for i in range(n):
        pairs += [(2 * i, 2 * ((i + 1) % n)), (2 * i + 1, 2 * ((i - 1) % n) + 1)]
    return lax.ppermute(message, (axis, "gz_1"), pairs)


def gather_sum(rows, axes):
    n = lax.axis_size(axes)
    wide = jnp.broadcast_to(rows[None], (n,) + rows.shape).reshape(n * rows.shape[0], rows.shape[1])
    wide = lax.all_to_all(wide, axes, 0, 0, tiled=True)
    return jnp.sum(wide.reshape((n,) + rows.shape), axis=0)


def total(rows):
    return gather_sum(gather_sum(rows, INNER), ("gx",))


def split(x):
    hi = x.astype(BF16)
    return hi, (x - hi.astype(F32)).astype(BF16)


def apply_block(mcat, vec):
    blk = mcat.shape[0]
    hi, lo = split(vec)
    out = jnp.dot(mcat, jnp.concatenate([hi, hi], axis=0), preferred_element_type=F32)
    return out + jnp.dot(mcat[:, :blk], lo, preferred_element_type=F32)


def column(row, blk):
    r = lax.broadcasted_iota(jnp.int32, (blk, blk), 0)
    c = lax.broadcasted_iota(jnp.int32, (blk, blk), 1)
    return jnp.sum(jnp.where(r == c, jnp.broadcast_to(row, (blk, blk)), 0.0), axis=1, keepdims=True)


def colsum(x):
    return jnp.sum(x, axis=0, keepdims=True)


def on_device(schur, interface_diag, precond, load, face_blocks):
    nblk, blk = precond.shape[3], precond.shape[4]
    cols = load.shape[-1]
    order = nblk * blk
    cap = face_blocks.shape[-1]
    slots = 6 * cap
    rows = cap * blk
    table = face_blocks.reshape(6, cap).T
    matrix = schur.reshape(order, order)
    diag = interface_diag.reshape(nblk, blk)

    def pick(table_ref, i):
        b = table_ref[i % cap, i // cap]
        return jnp.minimum(b, nblk - 1), (b < nblk).astype(F32)

    def pack(table_ref, load_ref, pre_ref, *refs):
        faces, (load_buf, pre_buf, load_sems, pre_sems) = refs[:6], refs[6:]
        copies = []
        for i in range(slots):
            b, _ = pick(table_ref, i)
            at = pl.multiple_of(b * blk, blk)
            copies.append(
                (
                    pltpu.make_async_copy(load_ref.at[pl.ds(at, blk), :], load_buf.at[i], load_sems.at[i]),
                    pltpu.make_async_copy(pre_ref.at[b], pre_buf.at[i], pre_sems.at[i]),
                )
            )
            for copy in copies[-1]:
                copy.start()
        for i in range(slots):
            _, m = pick(table_ref, i)
            d, at = i // cap, (i % cap) * blk
            for copy in copies[i]:
                copy.wait()
            faces[d][at : at + blk, :cols] = load_buf[i].astype(F32) * m
            faces[d][at : at + blk, cols:] = pre_buf[i] * m

    faces = call(
        pack,
        [((rows, cols + blk), F32)] * 6,
        (table, load.reshape(order, cols), precond.reshape(nblk, blk, blk)),
        scratch=(
            pltpu.VMEM((slots, blk, cols), BF16),
            pltpu.VMEM((slots, blk, blk), F32),
            pltpu.SemaphoreType.DMA((slots,)),
            pltpu.SemaphoreType.DMA((slots,)),
        ),
        raw=(1, 2),
    )
    came = [x for a in range(3) for x in exchange(faces[2 * a], faces[2 * a + 1], AXES[a])]

    def fetch(table_ref, matrix_ref, s_ref, sems):
        copies = []
        for i in range(slots):
            b, _ = pick(table_ref, i)
            copy = pltpu.make_async_copy(
                matrix_ref.at[pl.ds(pl.multiple_of(b * blk, blk), blk), :],
                s_ref.at[pl.ds(i * blk, blk), :],
                sems.at[i],
            )
            copy.start()
            copies.append(copy)
        for copy in copies:
            copy.wait()

    (sel,) = call(
        fetch,
        [((slots * blk, order), BF16)],
        (table, matrix),
        scratch=(pltpu.SemaphoreType.DMA((slots,)),),
        raw=(1,),
        flops=2 * 10**9,
    )

    def spread(table_ref, zb_ref, i, value):
        b = table_ref[i % cap, i // cap]

        @pl.when(b < nblk)
        def _():
            zb_ref[pl.ds(pl.multiple_of(b * blk, blk), blk), :] = value.astype(BF16)

    def local_schur(table_ref, d, s_ref, zb_ref, z_ref, diag_ref, out_ref):
        base = pl.multiple_of(d * rows, rows)
        product = jnp.dot(s_ref[pl.ds(base, rows), :], zb_ref[...], preferred_element_type=F32)
        for k in range(cap):
            b = table_ref[k, d]
            m = (b < nblk).astype(F32)
            dcol = column(diag_ref[pl.ds(jnp.minimum(b, nblk - 1), 1), :], blk)
            z = z_ref[pl.ds(base + k * blk, blk), :]
            out_ref[k * blk : (k + 1) * blk, :] = (product[k * blk : (k + 1) * blk] + dcol * z) * m

    long = slots * blk
    tall = (long, cols)
    flat = (rows, cols)

    def first(table_ref, *refs):
        own, got = refs[:6], refs[6:12]
        diag_ref, s_ref = refs[12:14]
        r_ref, z_ref, m_ref, zb_ref, up_ref, down_ref = refs[14:20]
        zb_ref[...] = jnp.zeros_like(zb_ref)
        for i in range(slots):
            d, at = i // cap, (i % cap) * blk
            r = own[d][at : at + blk, :cols] + got[d][at : at + blk, :cols]
            m = own[d][at : at + blk, cols:] + got[d][at : at + blk, cols:]
            hi, lo = split(m)
            mcat = jnp.concatenate([hi, lo], axis=1)
            m_ref[i * blk : (i + 1) * blk, :] = mcat
            r_ref[i * blk : (i + 1) * blk, :] = r
            z = apply_block(mcat, r)
            z_ref[i * blk : (i + 1) * blk, :] = z
            spread(table_ref, zb_ref, i, z)
        local_schur(table_ref, 0, s_ref, zb_ref, z_ref, diag_ref, up_ref)
        local_schur(table_ref, 1, s_ref, zb_ref, z_ref, diag_ref, down_ref)

    def pair(axis):
        def body(table_ref, zb_ref, z_ref, diag_ref, s_ref, up_ref, down_ref):
            local_schur(table_ref, 2 * axis, s_ref, zb_ref, z_ref, diag_ref, up_ref)
            local_schur(table_ref, 2 * axis + 1, s_ref, zb_ref, z_ref, diag_ref, down_ref)

        return body

    r, z1, mcat, zb, up, down = call(
        first,
        [(tall, F32), (tall, F32), ((long, 2 * blk), BF16), ((order, cols), BF16), (flat, F32), (flat, F32)],
        (table, *faces, *came, diag, sel),
        flops=2 * 10**9,
    )
    ys = [up, down]
    came = exchange(up, down, AXES[0])
    for a in (1, 2):
        up, down = call(
            pair(a), [(flat, F32)] * 2, (table, zb, z1, diag, sel), flops=10**9
        )
        ys += [up, down]
        came += exchange(up, down, AXES[a])

    def sides(axis):
        if axis == 2:
            return 4, 5
        low = lax.axis_index("gz_1") == 0
        return jnp.where(low, 2 * axis, 2 * axis + 1), jnp.where(low, 2 * axis + 1, 2 * axis)

    def second(table_ref, *refs):
        own, got = refs[:6], refs[6:12]
        m_ref, diag_ref, s_ref = refs[12:15]
        w_ref, z_ref, zb_ref, msg_ref, keep_ref = refs[15:20]
        zb_ref[...] = jnp.zeros_like(zb_ref)
        for i in range(slots):
            d, at = i // cap, (i % cap) * blk
            w = own[d][at : at + blk, :] + got[d][at : at + blk, :]
            w_ref[i * blk : (i + 1) * blk, :] = w
            z = apply_block(m_ref[i * blk : (i + 1) * blk, :], w)
            z_ref[i * blk : (i + 1) * blk, :] = z
            spread(table_ref, zb_ref, i, z)
        send, meet = sides(0)
        local_schur(table_ref, send, s_ref, zb_ref, z_ref, diag_ref, msg_ref)
        local_schur(table_ref, meet, s_ref, zb_ref, z_ref, diag_ref, keep_ref)

    def pair_once(axis):
        def body(table_ref, zb_ref, z_ref, diag_ref, s_ref, msg_ref, keep_ref):
            send, meet = sides(axis)
            local_schur(table_ref, send, s_ref, zb_ref, z_ref, diag_ref, msg_ref)
            local_schur(table_ref, meet, s_ref, zb_ref, z_ref, diag_ref, keep_ref)

        return body

    w1, z2, zb, msg, keep = call(
        second,
        [(tall, F32), (tall, F32), ((order, cols), BF16), (flat, F32), (flat, F32)],
        (table, *ys, *came, mcat, diag, sel),
        flops=2 * 10**9,
    )
    msgs, keeps = [msg], [keep]
    came = [exchange_once(msg, AXES[0])]
    for a in (1, 2):
        msg, keep = call(pair_once(a), [(flat, F32)] * 2, (table, zb, z2, diag, sel), flops=10**9)
        msgs.append(msg)
        keeps.append(keep)
        came.append(exchange_once(msg, AXES[a]))

    def dots(*refs):
        y_refs, msg_refs, keep_refs = refs[:6], refs[6:9], refs[9:12]
        r_ref, w_ref, out_ref = refs[12:15]
        sums = [jnp.zeros((1, cols), F32) for _ in range(5)]
        for d in range(6):
            r = r_ref[d * rows : (d + 1) * rows, :]
            w = w_ref[d * rows : (d + 1) * rows, :]
            sums[0] += 0.5 * colsum(r * r)
            sums[1] += colsum(r * y_refs[d][...])
            sums[2] += 0.5 * colsum(w * w)
        for a in range(3):
            for d, ref in zip(sides(a), (msg_refs[a], keep_refs[a])):
                at = pl.ds(pl.multiple_of(d * rows, rows), rows)
                y = ref[...]
                sums[3] += colsum(y * r_ref[at, :])
                sums[4] += colsum(y * w_ref[at, :])
        out_ref[...] = jnp.zeros_like(out_ref)
        for i in range(5):
            out_ref[i : i + 1, :] = sums[i]

    (sums,) = call(
        dots, [((8, cols), F32)], (*ys, *msgs, *keeps, r, w1), smem=0, flops=10**9
    )

    def norms(*refs):
        keep_refs, got, in_ref, out_ref = refs[:3], refs[3:6], refs[6], refs[7]
        out_ref[...] = in_ref[...]
        square = jnp.zeros((1, cols), F32)
        for a in range(3):
            both = keep_refs[a][...] + got[a][...]
            square += colsum(both * both)
        out_ref[5:6, :] = square

    (sums,) = call(norms, [((8, cols), F32)], (*keeps, *came, sums), smem=0)
    sums = total(sums)

    def finish(table_ref, z1_ref, z2_ref, gram_ref, out_ref, res_ref, z_buf, zero_buf, z_sems, zero_sems):
        def live_copy(i):
            b = table_ref[i % cap, i // cap]
            to = out_ref.at[pl.ds(pl.multiple_of(b * blk, blk), blk), :]
            return pltpu.make_async_copy(z_buf.at[i], to, z_sems.at[i])

        def dead_copy(b):
            return pltpu.make_async_copy(zero_buf, out_ref.at[pl.ds(b * blk, blk), :], zero_sems.at[b])

        zero_buf[...] = jnp.zeros_like(zero_buf)
        dead = []
        for b in range(nblk):
            hits = jnp.int32(0)
            for i in range(slots):
                hits += (table_ref[i % cap, i // cap] == b).astype(jnp.int32)
            dead.append(hits == 0)

            @pl.when(dead[b])
            def _():
                dead_copy(b).start()

        load_square = gram_ref[0:1, :]
        initial = jnp.sqrt(load_square + epsilon)
        rescale = 1.0 / initial
        scale2 = rescale * rescale
        h11 = gram_ref[1:2, :] * scale2
        b11 = gram_ref[2:3, :] * scale2
        c1v = gram_ref[3:4, :] * scale2
        c11 = gram_ref[4:5, :] * scale2
        e11 = gram_ref[5:6, :] * scale2
        g11 = load_square * scale2
        w_square = jnp.maximum(b11 - h11 * h11 * (2.0 - g11), 0.0)
        h21 = jnp.sqrt(w_square + epsilon)
        down = 1.0 / h21
        g22 = w_square * down * down
        g12 = h11 * (epsilon * scale2) * down
        h12 = (c1v - h11 * h11) * down
        dot22 = ((c11 - h11 * c1v) - h11 * (b11 - h11 * h11)) * down * down
        square = ((e11 - h11 * c11) - h11 * (c11 - h11 * b11)) * down * down
        h22 = dot22 - h12 * g12
        left = square - h12 * h12 * (2.0 - g11) - h22 * (2.0 * dot22 - h22 * g22) + 2.0 * h12 * h22 * g12
        h32 = jnp.sqrt(jnp.maximum(left, 0.0) + epsilon)
        r1 = jnp.sqrt(h11 * h11 + h21 * h21)
        c1, s1 = h11 / r1, h21 / r1
        top = c1 * h12 + s1 * h22
        bottom = c1 * h22 - s1 * h12
        r2 = jnp.sqrt(bottom * bottom + h32 * h32)
        c2, s2 = bottom / r2, h32 / r2
        y2 = -initial * s1 * c2 / r2
        y1 = (initial * c1 - top * y2) / r1
        res_ref[...] = initial * s1 * s2
        a2 = y2 * down * rescale
        a1 = y1 * rescale - a2 * h11
        for i in range(slots):
            z_buf[i] = a1 * z1_ref[i * blk : (i + 1) * blk, :] + a2 * z2_ref[i * blk : (i + 1) * blk, :]

            @pl.when(table_ref[i % cap, i // cap] < nblk)
            def _():
                live_copy(i).start()

        for b in range(nblk):

            @pl.when(dead[b])
            def _():
                dead_copy(b).wait()

        for i in range(slots):

            @pl.when(table_ref[i % cap, i // cap] < nblk)
            def _():
                live_copy(i).wait()

    out, res = call(
        finish,
        [((order, cols), F32), ((1, cols), F32)],
        (table, z1, z2, sums),
        scratch=(
            pltpu.VMEM((slots, blk, cols), F32),
            pltpu.VMEM((blk, cols), F32),
            pltpu.SemaphoreType.DMA((slots,)),
            pltpu.SemaphoreType.DMA((nblk,)),
        ),
        hbm_out=(0,),
    )
    return out.reshape(1, 1, 1, order, cols), res.reshape(cols)


def solution(mesh):
    torus = Mesh(
        mesh.devices.reshape(mesh.shape["gx"], mesh.shape["gy"], 4, 2), ("gx", "gy", "gz_0", "gz_1")
    )
    in_specs = (
        P("gx", "gy", GZ, None, None),
        P("gx", "gy", GZ, None),
        P("gx", "gy", GZ, None, None, None),
        P("gx", "gy", GZ, None, None),
        P("gx", "gy", GZ, None, None),
    )
    out_specs = (P("gx", "gy", GZ, None, None), P())
    return jax.shard_map(
        on_device, mesh=torus, in_specs=in_specs, out_specs=out_specs, check_vma=False
    )
```

```python
import functools

import jax
import jax.numpy as jnp
from jax import lax
from jax.experimental import pallas as pl
from jax.experimental.pallas import tpu as pltpu
from jax.sharding import Mesh
from jax.sharding import PartitionSpec as P

GZ = ("gz_0", "gz_1")
GROUP = 2
AXES = ("gx", "gy", GZ)
INNER = ("gy", "gz_0", "gz_1")


epsilon = 1e-06
TRUST = 1e-3
F32 = jnp.float32
BF16 = jnp.bfloat16


def call(body, outs, operands, scratch=(), smem=1, raw=(), flops=0, mib=16, flag=False):
    specs = []
    operands = list(operands)
    for i in range(len(operands)):
        if i < smem:
            specs.append(pl.BlockSpec(memory_space=pltpu.SMEM))
            operands[i] = pltpu.with_memory_space_constraint(operands[i], pltpu.HBM)
        elif i in raw:
            specs.append(pl.BlockSpec(memory_space=pltpu.HBM))
            operands[i] = pltpu.with_memory_space_constraint(operands[i], pltpu.HBM)
        else:
            specs.append(pl.BlockSpec(memory_space=pltpu.VMEM))
    return pl.pallas_call(
        body,
        out_shape=[jax.ShapeDtypeStruct(s, t) for s, t in outs]
        + [jax.ShapeDtypeStruct((1,), jnp.int32)] * flag,
        in_specs=specs,
        out_specs=[pl.BlockSpec(memory_space=pltpu.VMEM) for _ in outs]
        + [pl.BlockSpec(memory_space=pltpu.SMEM)] * flag,
        scratch_shapes=list(scratch),
        compiler_params=pltpu.CompilerParams(vmem_limit_bytes=mib * 2**20),
        cost_estimate=pl.CostEstimate(flops=flops, transcendentals=0, bytes_accessed=2**20),
    )(*operands)


def shifts(axis):
    n = lax.axis_size(axis)
    up = [(i, (i + 1) % n) for i in range(n)]
    return up, [(j, i) for i, j in up]


def exchange(to_next, to_previous, axis):
    up, down = shifts(axis)
    return [lax.ppermute(to_previous, axis, down), lax.ppermute(to_next, axis, up)]


def exchange_once(message, axis):
    if axis == GZ:
        return lax.ppermute(message, GZ, shifts(GZ)[0])
    n = lax.axis_size(axis)
    pairs = []
    for i in range(n):
        pairs += [(2 * i, 2 * ((i + 1) % n)), (2 * i + 1, 2 * ((i - 1) % n) + 1)]
    return lax.ppermute(message, (axis, "gz_1"), pairs)


def gather_sum(rows, axes):
    n = lax.axis_size(axes)
    wide = jnp.broadcast_to(rows[None], (n,) + rows.shape).reshape(n * rows.shape[0], rows.shape[1])
    wide = lax.all_to_all(wide, axes, 0, 0, tiled=True)
    return jnp.sum(wide.reshape((n,) + rows.shape), axis=0)


def total(rows):
    return gather_sum(gather_sum(rows, INNER), ("gx",))


def split(x):
    hi = x.astype(BF16)
    return hi, (x - hi.astype(F32)).astype(BF16)


def apply_block(mcat, vec):
    blk = mcat.shape[0]
    hi, lo = split(vec)
    out = jnp.dot(mcat, jnp.concatenate([hi, hi], axis=0), preferred_element_type=F32)
    return out + jnp.dot(mcat[:, :blk], lo, preferred_element_type=F32)


def column(row, blk):
    r = lax.broadcasted_iota(jnp.int32, (blk, blk), 0)
    c = lax.broadcasted_iota(jnp.int32, (blk, blk), 1)
    return jnp.sum(jnp.where(r == c, jnp.broadcast_to(row, (blk, blk)), 0.0), axis=1, keepdims=True)


def colsum(x):
    return jnp.sum(x, axis=0, keepdims=True)


def on_device(schur, interface_diag, precond, load, face_blocks):
    nblk, blk = precond.shape[3], precond.shape[4]
    cols = load.shape[-1]
    order = nblk * blk
    cap = face_blocks.shape[-1]
    slots = 6 * cap
    rows = cap * blk
    table = face_blocks.reshape(6, cap).T
    matrix = schur.reshape(order, order)
    diag = interface_diag.reshape(nblk, blk)

    def pick(table_ref, i):
        b = table_ref[i % cap, i // cap]
        return jnp.minimum(b, nblk - 1), (b < nblk).astype(F32)

    def pack():
        def body(table_ref, load_ref, pre_ref, *refs):
            outs = refs[:6]
            load_buf, pre_buf, load_sems, pre_sems = refs[6:]
            copies = []
            for i in range(slots):
                b, _ = pick(table_ref, i)
                at = pl.multiple_of(b * blk, blk)
                copies.append(
                    (
                        pltpu.make_async_copy(load_ref.at[pl.ds(at, blk), :], load_buf.at[i], load_sems.at[i]),
                        pltpu.make_async_copy(pre_ref.at[b], pre_buf.at[i], pre_sems.at[i]),
                    )
                )
                for copy in copies[-1]:
                    copy.start()
            for i in range(slots):
                _, m = pick(table_ref, i)
                out, at = outs[i // cap], (i % cap) * blk
                for copy in copies[i]:
                    copy.wait()
                out[at : at + blk, :cols] = load_buf[i].astype(F32) * m
                out[at : at + blk, cols:] = pre_buf[i] * m

        return call(
            body,
            [((rows, cols + blk), F32)] * 6,
            (table, load.reshape(order, cols), precond.reshape(nblk, blk, blk)),
            scratch=(
                pltpu.VMEM((slots, blk, cols), BF16),
                pltpu.VMEM((slots, blk, blk), F32),
                pltpu.SemaphoreType.DMA((slots,)),
                pltpu.SemaphoreType.DMA((slots,)),
            ),
            raw=(1, 2),
            flops=10**8,
        )

    faces = pack()
    came = [x for a in range(3) for x in exchange(faces[2 * a], faces[2 * a + 1], AXES[a])]

    def fetch(table_ref, matrix_ref, s_ref, sems):
        copies = []
        for i in range(slots):
            b, _ = pick(table_ref, i)
            copy = pltpu.make_async_copy(
                matrix_ref.at[pl.ds(pl.multiple_of(b * blk, blk), blk), :],
                s_ref.at[pl.ds(i * blk, blk), :],
                sems.at[i],
            )
            copy.start()
            copies.append(copy)
        for copy in copies:
            copy.wait()

    def live_rows():
        return call(
            fetch,
            [((slots * blk, order), BF16)],
            (table, matrix),
            scratch=(pltpu.SemaphoreType.DMA((slots,)),),
            raw=(1,),
            flops=2 * 10**9,
        )[0]

    sel = live_rows()

    def spread(table_ref, zb_ref, i, value):
        b = table_ref[i % cap, i // cap]

        @pl.when(b < nblk)
        def _():
            zb_ref[pl.ds(pl.multiple_of(b * blk, blk), blk), :] = value.astype(BF16)

    def local_schur(table_ref, s_ref, zb_ref, z_ref, diag_ref, outs):
        for g in range(0, 6, GROUP):
            product = jnp.dot(
                s_ref[g * rows : (g + GROUP) * rows, :], zb_ref[...], preferred_element_type=F32
            )
            for d in range(g, g + GROUP):
                for k in range(cap):
                    i = d * cap + k
                    b, m = pick(table_ref, i)
                    dcol = column(diag_ref[pl.ds(b, 1), :], blk)
                    z = z_ref[i * blk : (i + 1) * blk, :]
                    at = i * blk - g * rows
                    outs[d][k * blk : (k + 1) * blk, :] = (product[at : at + blk] + dcol * z) * m

    long = slots * blk
    tall = (long, cols)
    flat = (rows, cols)

    def first(table_ref, *refs):
        own, got = refs[:6], refs[6:12]
        diag_ref, s_ref = refs[12:14]
        r_ref, z_ref, m_ref = refs[14:17]
        y_refs, zb_ref = refs[17:23], refs[23]
        zb_ref[...] = jnp.zeros_like(zb_ref)
        for i in range(slots):
            d, at = i // cap, (i % cap) * blk
            r = own[d][at : at + blk, :cols] + got[d][at : at + blk, :cols]
            m = own[d][at : at + blk, cols:] + got[d][at : at + blk, cols:]
            hi, lo = split(m)
            mcat = jnp.concatenate([hi, lo], axis=1)
            m_ref[i * blk : (i + 1) * blk, :] = mcat
            r_ref[i * blk : (i + 1) * blk, :] = r
            z = apply_block(mcat, r)
            z_ref[i * blk : (i + 1) * blk, :] = z
            spread(table_ref, zb_ref, i, z)
        local_schur(table_ref, s_ref, zb_ref, z_ref, diag_ref, y_refs)

    spread_z = (pltpu.VMEM((order, cols), BF16),)
    r, z1, mcat, *ys = call(
        first,
        [(tall, F32), (tall, F32), ((long, 2 * blk), BF16)] + [(flat, F32)] * 6,
        (table, *faces, *came, diag, sel),
        scratch=spread_z,
        flops=2 * 10**9,
    )
    came = [x for a in range(3) for x in exchange(ys[2 * a], ys[2 * a + 1], AXES[a])]

    def sides(axis):
        if axis == 2:
            return 4, 5
        low = lax.axis_index("gz_1") == 0
        return jnp.where(low, 2 * axis, 2 * axis + 1), jnp.where(low, 2 * axis + 1, 2 * axis)

    def second(table_ref, *refs, given=False):
        if given:
            raw_ref, r_ref, gram_ref = refs[:3]
            scale = 1.0 / jnp.sqrt(gram_ref[0:1, :] + epsilon)
            h11 = gram_ref[1:2, :] * scale * scale
            refs = refs[3:]
        else:
            own, got = refs[:6], refs[6:12]
            refs = refs[12:]
        m_ref, diag_ref, s_ref = refs[:3]
        w_ref, z_ref = refs[3:5]
        msg_refs, keep_refs = refs[5:8], refs[8:11]
        refs = refs[11:]
        if given:
            first_ref, *refs = refs
        zb_ref, y_refs = refs[0], refs[1:7]
        zb_ref[...] = jnp.zeros_like(zb_ref)
        for i in range(slots):
            d, at = i // cap, (i % cap) * blk
            if given:
                w = raw_ref[i * blk : (i + 1) * blk, :] - h11 * r_ref[i * blk : (i + 1) * blk, :]
                w = w * scale
                r = r_ref[i * blk : (i + 1) * blk, :]
                first_ref[i * blk : (i + 1) * blk, :] = apply_block(m_ref[i * blk : (i + 1) * blk, :], r)
            else:
                w = own[d][at : at + blk, :] + got[d][at : at + blk, :]
            w_ref[i * blk : (i + 1) * blk, :] = w
            z = apply_block(m_ref[i * blk : (i + 1) * blk, :], w)
            z_ref[i * blk : (i + 1) * blk, :] = z
            spread(table_ref, zb_ref, i, z)
        local_schur(table_ref, s_ref, zb_ref, z_ref, diag_ref, y_refs)
        low = lax.axis_index("gz_1") == 0
        for a in range(2):

            @pl.when(low)
            def _():
                msg_refs[a][...] = y_refs[2 * a][...]
                keep_refs[a][...] = y_refs[2 * a + 1][...]

            @pl.when(jnp.logical_not(low))
            def _():
                msg_refs[a][...] = y_refs[2 * a + 1][...]
                keep_refs[a][...] = y_refs[2 * a][...]

        msg_refs[2][...] = y_refs[4][...]
        keep_refs[2][...] = y_refs[5][...]

    def dots(*refs):
        y_refs, msg_refs, keep_refs = refs[:6], refs[6:9], refs[9:12]
        r_ref, w_ref, out_ref = refs[12:15]
        sums = [jnp.zeros((1, cols), F32) for _ in range(5)]
        for d in range(6):
            r = r_ref[d * rows : (d + 1) * rows, :]
            w = w_ref[d * rows : (d + 1) * rows, :]
            sums[0] += 0.5 * colsum(r * r)
            sums[1] += colsum(r * y_refs[d][...])
            sums[2] += 0.5 * colsum(w * w)
        for a in range(3):
            for d, ref in zip(sides(a), (msg_refs[a], keep_refs[a])):
                at = pl.ds(pl.multiple_of(d * rows, rows), rows)
                y = ref[...]
                sums[3] += colsum(y * r_ref[at, :])
                sums[4] += colsum(y * w_ref[at, :])
        out_ref[...] = jnp.zeros_like(out_ref)
        for i in range(5):
            out_ref[i : i + 1, :] = sums[i]

    def norms(*refs):
        keep_refs, got, in_ref, out_ref = refs[:3], refs[3:6], refs[6], refs[7]
        out_ref[...] = in_ref[...]
        square = jnp.zeros((1, cols), F32)
        for a in range(3):
            both = keep_refs[a][...] + got[a][...]
            square += colsum(both * both)
        out_ref[5:6, :] = square

    def second_step(ys, heads, mcat, sel, r, given=False):
        w, z, *rest = call(
            functools.partial(second, given=given),
            [(tall, F32), (tall, F32)] + [(flat, F32)] * 6 + [(tall, F32)] * given,
            (table, *heads, mcat, diag, sel),
            scratch=spread_z + (pltpu.VMEM(flat, F32),) * 6,
            flops=2 * 10**9,
        )
        msgs, keeps, z1 = rest[:3], rest[3:6], rest[6:]
        got = []
        for a in range(3):
            got.append(exchange_once(msgs[a], AXES[a]))
        (sums,) = call(dots, [((8, cols), F32)], (*ys, *msgs, *keeps, r, w), smem=0, flops=10**9)
        (sums,) = call(norms, [((8, cols), F32)], (*keeps, *got, sums), smem=0)
        return w, z, total(sums), z1

    w1, z2, sums, _ = second_step(ys, (*ys, *came), mcat, sel, r)

    def weights(initial, h11, h21, h12, h22, h32):
        r1 = jnp.sqrt(h11 * h11 + h21 * h21)
        c1, s1 = h11 / r1, h21 / r1
        top = c1 * h12 + s1 * h22
        bottom = c1 * h22 - s1 * h12
        r2 = jnp.sqrt(bottom * bottom + h32 * h32)
        c2, s2 = bottom / r2, h32 / r2
        y2 = -initial * s1 * c2 / r2
        y1 = (initial * c1 - top * y2) / r1
        return y1, y2, initial * s1 * s2

    def gram_rest(square, h12, dot22, g11, g12, g22):
        h22 = dot22 - h12 * g12
        left = square - h12 * h12 * (2.0 - g11) - h22 * (2.0 * dot22 - h22 * g22)
        return h22, left + 2.0 * h12 * h22 * g12

    def store(table_ref, z1_ref, z2_ref, a1, a2, out_ref):
        out_ref[...] = jnp.zeros_like(out_ref)
        for i in range(slots):
            b = table_ref[i % cap, i // cap]

            @pl.when(b < nblk)
            def _():
                z = a1 * z1_ref[i * blk : (i + 1) * blk, :] + a2 * z2_ref[i * blk : (i + 1) * blk, :]
                out_ref[pl.ds(pl.multiple_of(b * blk, blk), blk), :] = z

    def finish(table_ref, z1_ref, z2_ref, gram_ref, out_ref, res_ref, flag_ref):
        load_square = gram_ref[0:1, :]
        initial = jnp.sqrt(load_square + epsilon)
        rescale = 1.0 / initial
        scale2 = rescale * rescale
        h11 = gram_ref[1:2, :] * scale2
        b11 = gram_ref[2:3, :] * scale2
        c1v = gram_ref[3:4, :] * scale2
        c11 = gram_ref[4:5, :] * scale2
        e11 = gram_ref[5:6, :] * scale2
        g11 = load_square * scale2
        w_square = jnp.maximum(b11 - h11 * h11 * (2.0 - g11), 0.0)
        h21 = jnp.sqrt(w_square + epsilon)
        down = 1.0 / h21
        g22 = w_square * down * down
        g12 = h11 * (epsilon * scale2) * down
        h12 = (c1v - h11 * h11) * down
        dot22 = ((c11 - h11 * c1v) - h11 * (b11 - h11 * h11)) * down * down
        square = ((e11 - h11 * c11) - h11 * (c11 - h11 * b11)) * down * down
        h22, left = gram_rest(square, h12, dot22, g11, g12, g22)
        h32 = jnp.sqrt(jnp.maximum(left, 0.0) + epsilon)
        y1, y2, res = weights(initial, h11, h21, h12, h22, h32)
        a2 = y2 * down * rescale
        res_ref[...] = res
        store(table_ref, z1_ref, z2_ref, y1 * rescale - a2 * h11, a2, out_ref)
        kept = (w_square >= TRUST * b11) & (left * (w_square + epsilon) >= TRUST * e11)
        flag_ref[0] = 1 - jnp.min(kept.astype(F32)).astype(jnp.int32)

    def finish_again(table_ref, z1_ref, z2_ref, one_ref, two_ref, out_ref, res_ref):
        load_square = one_ref[0:1, :]
        initial = jnp.sqrt(load_square + epsilon)
        rescale = 1.0 / initial
        h11 = one_ref[1:2, :] * rescale * rescale
        w_square = two_ref[2:3, :]
        h21 = jnp.sqrt(w_square + epsilon)
        down = 1.0 / h21
        g11 = load_square * rescale * rescale
        g22 = w_square * down * down
        g12 = h11 * (epsilon * rescale * rescale) * down
        h12 = two_ref[3:4, :] * rescale * down
        dot22 = two_ref[4:5, :] * down * down
        square = two_ref[5:6, :] * down * down
        h22, left = gram_rest(square, h12, dot22, g11, g12, g22)
        h32 = jnp.sqrt(jnp.maximum(left, 0.0) + epsilon)
        y1, y2, res = weights(initial, h11, h21, h12, h22, h32)
        res_ref[...] = res
        store(table_ref, z1_ref, z2_ref, y1 * rescale, y2 * down, out_ref)

    results = [((order, cols), F32), ((1, cols), F32)]
    out, res, flag = call(finish, results, (table, z1, z2, sums), flag=True)

    def careful(state):
        r, w1, mcat = (pltpu.with_memory_space_constraint(x, pltpu.HBM) for x in state[3:6])
        sums = state[6]
        zeros = [jnp.zeros(flat, F32)] * 6
        _, z2, more, (z1,) = second_step(zeros, (w1, r, sums), mcat, live_rows(), r, given=True)
        out, res = call(finish_again, results, (table, z1, z2, sums, more))
        return jnp.zeros((1,), jnp.int32), out, res, *state[3:]

    _, out, res, *_ = lax.while_loop(
        lambda state: state[0][0] > 0, careful, (flag, out, res, r, w1, mcat, sums)
    )
    return out.reshape(1, 1, 1, order, cols), res.reshape(cols)


def solution(mesh):
    torus = Mesh(
        mesh.devices.reshape(mesh.shape["gx"], mesh.shape["gy"], 4, 2), ("gx", "gy", "gz_0", "gz_1")
    )
    in_specs = (
        P("gx", "gy", GZ, None, None),
        P("gx", "gy", GZ, None),
        P("gx", "gy", GZ, None, None, None),
        P("gx", "gy", GZ, None, None),
        P("gx", "gy", GZ, None, None),
    )
    out_specs = (P("gx", "gy", GZ, None, None), P())
    return jax.shard_map(
        on_device, mesh=torus, in_specs=in_specs, out_specs=out_specs, check_vma=False
    )
```

```python
import functools

import jax
import jax.numpy as jnp
from jax import lax
from jax.experimental import pallas as pl
from jax.experimental.pallas import tpu as pltpu
from jax.sharding import Mesh
from jax.sharding import PartitionSpec as P

GZ = ("gz_0", "gz_1")
STEPS = 4
AXES = ("gx", "gy", GZ)
INNER = ("gy", "gz_0", "gz_1")


epsilon = 1e-06
TRUST = 1e-3
F32 = jnp.float32
BF16 = jnp.bfloat16


def call(body, outs, operands, scratch=(), smem=1, raw=(), flops=0, mib=16, hbm_table=False):
    specs = []
    operands = list(operands)
    for i in range(len(operands)):
        if i < smem:
            specs.append(pl.BlockSpec(memory_space=pltpu.SMEM))
            if hbm_table:
                operands[i] = pltpu.with_memory_space_constraint(operands[i], pltpu.HBM)
        elif i in raw:
            specs.append(pl.BlockSpec(memory_space=pltpu.HBM))
            operands[i] = pltpu.with_memory_space_constraint(operands[i], pltpu.HBM)
        else:
            specs.append(pl.BlockSpec(memory_space=pltpu.VMEM))
    return pl.pallas_call(
        body,
        out_shape=[jax.ShapeDtypeStruct(s, t) for s, t in outs],
        in_specs=specs,
        out_specs=[pl.BlockSpec(memory_space=pltpu.VMEM) for _ in outs],
        scratch_shapes=list(scratch),
        compiler_params=pltpu.CompilerParams(vmem_limit_bytes=mib * 2**20),
        cost_estimate=pl.CostEstimate(flops=flops, transcendentals=0, bytes_accessed=2**20),
    )(*operands)


def shifts(axis):
    n = lax.axis_size(axis)
    up = [(i, (i + 1) % n) for i in range(n)]
    return up, [(j, i) for i, j in up]


def exchange(to_next, to_previous, axis):
    up, down = shifts(axis)
    return [lax.ppermute(to_previous, axis, down), lax.ppermute(to_next, axis, up)]


def exchange_once(message, axis):
    if axis == GZ:
        return lax.ppermute(message, GZ, shifts(GZ)[0])
    n = lax.axis_size(axis)
    pairs = []
    for i in range(n):
        pairs += [(2 * i, 2 * ((i + 1) % n)), (2 * i + 1, 2 * ((i - 1) % n) + 1)]
    return lax.ppermute(message, (axis, "gz_1"), pairs)


def gather_sum(rows, axes):
    n = lax.axis_size(axes)
    wide = jnp.broadcast_to(rows[None], (n,) + rows.shape).reshape(n * rows.shape[0], rows.shape[1])
    wide = lax.all_to_all(wide, axes, 0, 0, tiled=True)
    return jnp.sum(wide.reshape((n,) + rows.shape), axis=0)


def total(rows):
    return gather_sum(gather_sum(rows, INNER), ("gx",))


def split(x):
    hi = x.astype(BF16)
    return hi, (x - hi.astype(F32)).astype(BF16)


def apply_block(mcat, vec):
    blk = mcat.shape[0]
    hi, lo = split(vec)
    out = jnp.dot(mcat, jnp.concatenate([hi, hi], axis=0), preferred_element_type=F32)
    return out + jnp.dot(mcat[:, :blk], lo, preferred_element_type=F32)


def column(row, blk):
    r = lax.broadcasted_iota(jnp.int32, (blk, blk), 0)
    c = lax.broadcasted_iota(jnp.int32, (blk, blk), 1)
    return jnp.sum(jnp.where(r == c, jnp.broadcast_to(row, (blk, blk)), 0.0), axis=1, keepdims=True)


def colsum(x):
    return jnp.sum(x, axis=0, keepdims=True)


def on_device(schur, interface_diag, precond, load, face_blocks):
    nblk, blk = precond.shape[3], precond.shape[4]
    cols = load.shape[-1]
    order = nblk * blk
    cap = face_blocks.shape[-1]
    slots = 6 * cap
    rows = cap * blk
    table = face_blocks.reshape(6, cap).T
    matrix = schur.reshape(order, order)
    diag = interface_diag.reshape(nblk, blk)

    def pick(table_ref, i):
        b = table_ref[i % cap, i // cap]
        return jnp.minimum(b, nblk - 1), (b < nblk).astype(F32)

    def pack():
        def body(table_ref, load_ref, pre_ref, *refs):
            outs = refs[:6]
            load_buf, pre_buf, load_sems, pre_sems = refs[6:]
            copies = []
            for i in range(slots):
                b, _ = pick(table_ref, i)
                at = pl.multiple_of(b * blk, blk)
                copies.append(
                    (
                        pltpu.make_async_copy(load_ref.at[pl.ds(at, blk), :], load_buf.at[i], load_sems.at[i]),
                        pltpu.make_async_copy(pre_ref.at[b], pre_buf.at[i], pre_sems.at[i]),
                    )
                )
                for copy in copies[-1]:
                    copy.start()
            for i in range(slots):
                _, m = pick(table_ref, i)
                out, at = outs[i // cap], (i % cap) * blk
                for copy in copies[i]:
                    copy.wait()
                out[at : at + blk, :cols] = load_buf[i].astype(F32) * m
                out[at : at + blk, cols:] = pre_buf[i] * m

        return call(
            body,
            [((rows, cols + blk), F32)] * 6,
            (table, load.reshape(order, cols), precond.reshape(nblk, blk, blk)),
            scratch=(
                pltpu.VMEM((slots, blk, cols), BF16),
                pltpu.VMEM((slots, blk, blk), F32),
                pltpu.SemaphoreType.DMA((slots,)),
                pltpu.SemaphoreType.DMA((slots,)),
            ),
            raw=(1, 2),
            flops=10**8,
            hbm_table=True,
        )

    faces = pack()
    came = [x for a in range(3) for x in exchange(faces[2 * a], faces[2 * a + 1], AXES[a])]

    def fetch(table_ref, matrix_ref, s_ref, row_buf, sems):
        copies = []
        for i in range(slots):
            b, _ = pick(table_ref, i)
            copy = pltpu.make_async_copy(
                matrix_ref.at[pl.ds(pl.multiple_of(b * blk, blk), blk), :],
                row_buf.at[pl.ds(i * blk, blk), :],
                sems.at[i],
            )
            copy.start()
            copies.append(copy)
        for i in range(slots):
            copies[i].wait()
            for j in range(slots):
                b, _ = pick(table_ref, j)
                s_ref[i * blk : (i + 1) * blk, j * blk : (j + 1) * blk] = row_buf[
                    i * blk : (i + 1) * blk, pl.ds(pl.multiple_of(b * blk, blk), blk)
                ]

    def live_part():
        return call(
            fetch,
            [((slots * blk, slots * blk), BF16)],
            (table, matrix),
            scratch=(pltpu.VMEM((slots * blk, order), BF16), pltpu.SemaphoreType.DMA((slots,))),
            raw=(1,),
            flops=2 * 10**9,
        )[0]

    sel = live_part()

    def local_schur(table_ref, d, s_ref, zb_ref, z_ref, diag_ref, out_ref):
        base = d * rows if isinstance(d, int) else pl.multiple_of(d * rows, rows)
        product = jnp.dot(s_ref[pl.ds(base, rows), :], zb_ref[...], preferred_element_type=F32)
        for k in range(cap):
            b = table_ref[k, d]
            m = (b < nblk).astype(F32)
            dcol = column(diag_ref[pl.ds(jnp.minimum(b, nblk - 1), 1), :], blk)
            z = z_ref[pl.ds(base + k * blk, blk), :]
            out_ref[k * blk : (k + 1) * blk, :] = (product[k * blk : (k + 1) * blk] + dcol * z) * m

    long = slots * blk
    tall = (long, cols)
    flat = (rows, cols)

    def first(table_ref, *refs):
        own, got = refs[:6], refs[6:12]
        diag_ref, s_ref = refs[12:14]
        r_ref, z_ref, m_ref = refs[14:17]
        y_refs, zb_ref = refs[17:23], refs[23]
        for i in range(slots):
            d, at = i // cap, (i % cap) * blk
            r = own[d][at : at + blk, :cols] + got[d][at : at + blk, :cols]
            m = own[d][at : at + blk, cols:] + got[d][at : at + blk, cols:]
            hi, lo = split(m)
            mcat = jnp.concatenate([hi, lo], axis=1)
            m_ref[i * blk : (i + 1) * blk, :] = mcat
            r_ref[i * blk : (i + 1) * blk, :] = r
            z = apply_block(mcat, r)
            z_ref[i * blk : (i + 1) * blk, :] = z
            zb_ref[i * blk : (i + 1) * blk, :] = z.astype(BF16)
        for d in range(6):
            local_schur(table_ref, d, s_ref, zb_ref, z_ref, diag_ref, y_refs[d])

    r, z1, mcat, *ys = call(
        first,
        [(tall, F32), (tall, F32), ((long, 2 * blk), BF16)] + [(flat, F32)] * 6,
        (table, *faces, *came, diag, sel),
        scratch=(pltpu.VMEM(tall, BF16),),
        flops=2 * 10**9,
    )
    came = [x for a in range(3) for x in exchange(ys[2 * a], ys[2 * a + 1], AXES[a])]

    def sides(axis):
        if axis == 2:
            return 4, 5
        low = lax.axis_index("gz_1") == 0
        return jnp.where(low, 2 * axis, 2 * axis + 1), jnp.where(low, 2 * axis + 1, 2 * axis)

    def second(table_ref, *refs, given=False):
        if given:
            raw_ref, r_ref, gram_ref = refs[:3]
            scale = 1.0 / jnp.sqrt(gram_ref[0:1, :] + epsilon)
            h11 = gram_ref[1:2, :] * scale * scale
            refs = refs[3:]
        else:
            own, got = refs[:6], refs[6:12]
            refs = refs[12:]
        m_ref, diag_ref, s_ref = refs[:3]
        w_ref, z_ref, zb_ref = refs[3:6]
        msg_refs = refs[6:9]
        for i in range(slots):
            d, at = i // cap, (i % cap) * blk
            if given:
                w = raw_ref[i * blk : (i + 1) * blk, :] - h11 * r_ref[i * blk : (i + 1) * blk, :]
                w = w * scale
                r = r_ref[i * blk : (i + 1) * blk, :]
                refs[9][i * blk : (i + 1) * blk, :] = apply_block(m_ref[i * blk : (i + 1) * blk, :], r)
            else:
                w = own[d][at : at + blk, :] + got[d][at : at + blk, :]
            w_ref[i * blk : (i + 1) * blk, :] = w
            z = apply_block(m_ref[i * blk : (i + 1) * blk, :], w)
            z_ref[i * blk : (i + 1) * blk, :] = z
            zb_ref[i * blk : (i + 1) * blk, :] = z.astype(BF16)
        for a in range(3):
            local_schur(table_ref, sides(a)[0], s_ref, zb_ref, z_ref, diag_ref, msg_refs[a])

    def rest_of_second(table_ref, zb_ref, z_ref, diag_ref, s_ref, *keep_refs):
        for a in range(3):
            local_schur(table_ref, sides(a)[1], s_ref, zb_ref, z_ref, diag_ref, keep_refs[a])

    def dots(*refs):
        y_refs, msg_refs, keep_refs = refs[:6], refs[6:9], refs[9:12]
        r_ref, w_ref, out_ref = refs[12:15]
        sums = [jnp.zeros((1, cols), F32) for _ in range(5)]
        for d in range(6):
            r = r_ref[d * rows : (d + 1) * rows, :]
            w = w_ref[d * rows : (d + 1) * rows, :]
            sums[0] += 0.5 * colsum(r * r)
            sums[1] += colsum(r * y_refs[d][...])
            sums[2] += 0.5 * colsum(w * w)
        for a in range(3):
            for d, ref in zip(sides(a), (msg_refs[a], keep_refs[a])):
                at = pl.ds(pl.multiple_of(d * rows, rows), rows)
                y = ref[...]
                sums[3] += colsum(y * r_ref[at, :])
                sums[4] += colsum(y * w_ref[at, :])
        out_ref[...] = jnp.zeros_like(out_ref)
        for i in range(5):
            out_ref[i : i + 1, :] = sums[i]

    def norms(*refs):
        keep_refs, got, in_ref, out_ref = refs[:3], refs[3:6], refs[6], refs[7]
        out_ref[...] = in_ref[...]
        square = jnp.zeros((1, cols), F32)
        for a in range(3):
            both = keep_refs[a][...] + got[a][...]
            square += colsum(both * both)
        out_ref[5:6, :] = square

    def second_step(ys, heads, mcat, sel, r, given=False):
        w, z, zb, *rest = call(
            functools.partial(second, given=given),
            [(tall, F32), (tall, F32), (tall, BF16)] + [(flat, F32)] * 3 + [(tall, F32)] * given,
            (table, *heads, mcat, diag, sel),
            flops=2 * 10**9,
        )
        msgs, z1 = rest[:3], rest[3:]
        got = []
        for a in range(3):
            got.append(exchange_once(msgs[a], AXES[a]))
        keeps = call(
            rest_of_second, [(flat, F32)] * 3, (table, zb, z, diag, sel), flops=10**9
        )
        (sums,) = call(dots, [((8, cols), F32)], (*ys, *msgs, *keeps, r, w), smem=0, flops=10**9)
        (sums,) = call(norms, [((8, cols), F32)], (*keeps, *got, sums), smem=0)
        return w, z, total(sums), z1

    w1, z2, sums, _ = second_step(ys, (*ys, *came), mcat, sel, r)

    def weights(initial, h11, h21, h12, h22, h32):
        r1 = jnp.sqrt(h11 * h11 + h21 * h21)
        c1, s1 = h11 / r1, h21 / r1
        top = c1 * h12 + s1 * h22
        bottom = c1 * h22 - s1 * h12
        r2 = jnp.sqrt(bottom * bottom + h32 * h32)
        c2, s2 = bottom / r2, h32 / r2
        y2 = -initial * s1 * c2 / r2
        y1 = (initial * c1 - top * y2) / r1
        return y1, y2, initial * s1 * s2

    def gram_rest(square, h12, dot22, g11, g12, g22):
        h22 = dot22 - h12 * g12
        left = square - h12 * h12 * (2.0 - g11) - h22 * (2.0 * dot22 - h22 * g22)
        return h22, left + 2.0 * h12 * h22 * g12

    def store(table_ref, z1_ref, z2_ref, a1, a2, out_ref):
        out_ref[...] = jnp.zeros_like(out_ref)
        for i in range(slots):
            b = table_ref[i % cap, i // cap]

            @pl.when(b < nblk)
            def _():
                z = a1 * z1_ref[i * blk : (i + 1) * blk, :] + a2 * z2_ref[i * blk : (i + 1) * blk, :]
                out_ref[pl.ds(pl.multiple_of(b * blk, blk), blk), :] = z

    def finish(table_ref, z1_ref, z2_ref, gram_ref, out_ref, res_ref, flag_ref, slot_ref, buf_ref, sems):
        for b in range(nblk):
            slot_ref[b] = jnp.int32(-1)
        for i in range(slots):
            slot_ref[table_ref[i % cap, i // cap]] = jnp.int32(i)
        load_square = gram_ref[0:1, :]
        initial = jnp.sqrt(load_square + epsilon)
        rescale = 1.0 / initial
        scale2 = rescale * rescale
        h11 = gram_ref[1:2, :] * scale2
        b11 = gram_ref[2:3, :] * scale2
        c1v = gram_ref[3:4, :] * scale2
        c11 = gram_ref[4:5, :] * scale2
        e11 = gram_ref[5:6, :] * scale2
        g11 = load_square * scale2
        w_square = jnp.maximum(b11 - h11 * h11 * (2.0 - g11), 0.0)
        h21 = jnp.sqrt(w_square + epsilon)
        down = 1.0 / h21
        g22 = w_square * down * down
        g12 = h11 * (epsilon * scale2) * down
        h12 = (c1v - h11 * h11) * down
        dot22 = ((c11 - h11 * c1v) - h11 * (b11 - h11 * h11)) * down * down
        square = ((e11 - h11 * c11) - h11 * (c11 - h11 * b11)) * down * down
        h22, left = gram_rest(square, h12, dot22, g11, g12, g22)
        h32 = jnp.sqrt(jnp.maximum(left, 0.0) + epsilon)
        y1, y2, res = weights(initial, h11, h21, h12, h22, h32)
        a2 = y2 * down * rescale
        res_ref[...] = res
        a1 = y1 * rescale - a2 * h11
        copies = []
        for g in range(STEPS):
            for b in range(g * nblk // STEPS, (g + 1) * nblk // STEPS):
                slot = slot_ref[b]
                m = (slot >= 0).astype(F32)
                at = pl.ds(pl.multiple_of(jnp.maximum(slot, 0) * blk, blk), blk)
                z = (a1 * m) * z1_ref[at, :] + (a2 * m) * z2_ref[at, :]
                buf_ref[b * blk : (b + 1) * blk, :] = z
            part = pl.ds(g * (order // STEPS), order // STEPS)
            copies.append(pltpu.make_async_copy(buf_ref.at[part, :], out_ref.at[part, :], sems.at[g]))
            copies[-1].start()
        kept = (w_square >= TRUST * b11) & (left * (w_square + epsilon) >= TRUST * e11)
        flag_ref[0] = 1 - jnp.min(kept.astype(F32)).astype(jnp.int32)
        for copy in copies:
            copy.wait()

    def finish_again(table_ref, z1_ref, z2_ref, one_ref, two_ref, out_ref, res_ref):
        load_square = one_ref[0:1, :]
        initial = jnp.sqrt(load_square + epsilon)
        rescale = 1.0 / initial
        h11 = one_ref[1:2, :] * rescale * rescale
        w_square = two_ref[2:3, :]
        h21 = jnp.sqrt(w_square + epsilon)
        down = 1.0 / h21
        g11 = load_square * rescale * rescale
        g22 = w_square * down * down
        g12 = h11 * (epsilon * rescale * rescale) * down
        h12 = two_ref[3:4, :] * rescale * down
        dot22 = two_ref[4:5, :] * down * down
        square = two_ref[5:6, :] * down * down
        h22, left = gram_rest(square, h12, dot22, g11, g12, g22)
        h32 = jnp.sqrt(jnp.maximum(left, 0.0) + epsilon)
        y1, y2, res = weights(initial, h11, h21, h12, h22, h32)
        res_ref[...] = res
        store(table_ref, z1_ref, z2_ref, y1 * rescale, y2 * down, out_ref)

    results = [((order, cols), F32), ((1, cols), F32)]
    out, res, flag = pl.pallas_call(
        finish,
        out_shape=[jax.ShapeDtypeStruct(shape, t) for shape, t in results]
        + [jax.ShapeDtypeStruct((1,), jnp.int32)],
        in_specs=[pl.BlockSpec(memory_space=pltpu.SMEM)] + [pl.BlockSpec(memory_space=pltpu.VMEM)] * 3,
        out_specs=[
            pl.BlockSpec(memory_space=pltpu.HBM),
            pl.BlockSpec(memory_space=pltpu.VMEM),
            pl.BlockSpec(memory_space=pltpu.SMEM),
        ],
        scratch_shapes=[
            pltpu.SMEM((nblk + 1,), jnp.int32),
            pltpu.VMEM((order, cols), F32),
            pltpu.SemaphoreType.DMA((STEPS,)),
        ],
        compiler_params=pltpu.CompilerParams(vmem_limit_bytes=16 * 2**20),
    )(table, z1, z2, sums)

    def careful(state):
        r, w1, mcat = (pltpu.with_memory_space_constraint(x, pltpu.HBM) for x in state[3:6])
        sums = state[6]
        zeros = [jnp.zeros(flat, F32)] * 6
        _, z2, more, (z1,) = second_step(zeros, (w1, r, sums), mcat, live_part(), r, given=True)
        out, res = call(finish_again, results, (table, z1, z2, sums, more))
        return jnp.zeros((1,), jnp.int32), out, res, *state[3:]

    _, out, res, *_ = lax.while_loop(
        lambda state: state[0][0] > 0, careful, (flag, out, res, r, w1, mcat, sums)
    )
    return out.reshape(1, 1, 1, order, cols), res.reshape(cols)


def solution(mesh):
    torus = Mesh(
        mesh.devices.reshape(mesh.shape["gx"], mesh.shape["gy"], 4, 2), ("gx", "gy", "gz_0", "gz_1")
    )
    in_specs = (
        P("gx", "gy", GZ, None, None),
        P("gx", "gy", GZ, None),
        P("gx", "gy", GZ, None, None, None),
        P("gx", "gy", GZ, None, None),
        P("gx", "gy", GZ, None, None),
    )
    out_specs = (P("gx", "gy", GZ, None, None), P())
    return jax.shard_map(
        on_device, mesh=torus, in_specs=in_specs, out_specs=out_specs, check_vma=False
    )
```

```python
import functools

import jax
import jax.numpy as jnp
from jax import lax
from jax.experimental import pallas as pl
from jax.experimental.pallas import tpu as pltpu
from jax.sharding import Mesh
from jax.sharding import PartitionSpec as P

GZ = ("gz_0", "gz_1")
STEPS = 4
AXES = ("gx", "gy", GZ)
INNER = ("gy", "gz_0", "gz_1")


epsilon = 1e-06
TRUST = 1e-3
F32 = jnp.float32
BF16 = jnp.bfloat16


def call(body, outs, operands, scratch=(), smem=1, raw=(), flops=0, mib=16, hbm_table=False):
    specs = []
    operands = list(operands)
    for i in range(len(operands)):
        if i < smem:
            specs.append(pl.BlockSpec(memory_space=pltpu.SMEM))
            if hbm_table:
                operands[i] = pltpu.with_memory_space_constraint(operands[i], pltpu.HBM)
        elif i in raw:
            specs.append(pl.BlockSpec(memory_space=pltpu.HBM))
            operands[i] = pltpu.with_memory_space_constraint(operands[i], pltpu.HBM)
        else:
            specs.append(pl.BlockSpec(memory_space=pltpu.VMEM))
    return pl.pallas_call(
        body,
        out_shape=[jax.ShapeDtypeStruct(s, t) for s, t in outs],
        in_specs=specs,
        out_specs=[pl.BlockSpec(memory_space=pltpu.VMEM) for _ in outs],
        scratch_shapes=list(scratch),
        compiler_params=pltpu.CompilerParams(vmem_limit_bytes=mib * 2**20),
        cost_estimate=pl.CostEstimate(flops=flops, transcendentals=0, bytes_accessed=2**20),
    )(*operands)


def shifts(axis):
    n = lax.axis_size(axis)
    up = [(i, (i + 1) % n) for i in range(n)]
    return up, [(j, i) for i, j in up]


def exchange(to_next, to_previous, axis):
    if axis == GZ:
        n = lax.axis_size(GZ)
        across = lax.ppermute(to_previous, GZ, [(i, (i - 1 + 2 * (i % 2)) % n) for i in range(n)])
        return [lax.ppermute(to_next, GZ, [(i, i ^ 1) for i in range(n)]), across]
    up, down = shifts(axis)
    return [lax.ppermute(to_previous, axis, down), lax.ppermute(to_next, axis, up)]


def exchange_once(message, axis):
    if axis == GZ:
        return lax.ppermute(message, GZ, shifts(GZ)[0])
    n = lax.axis_size(axis)
    pairs = []
    for i in range(n):
        pairs += [(2 * i, 2 * ((i + 1) % n)), (2 * i + 1, 2 * ((i - 1) % n) + 1)]
    return lax.ppermute(message, (axis, "gz_1"), pairs)


def gather_sum(rows, axes):
    n = lax.axis_size(axes)
    wide = jnp.broadcast_to(rows[None], (n,) + rows.shape).reshape(n * rows.shape[0], rows.shape[1])
    wide = lax.all_to_all(wide, axes, 0, 0, tiled=True)
    return jnp.sum(wide.reshape((n,) + rows.shape), axis=0)


def total(rows):
    return gather_sum(gather_sum(rows, INNER), ("gx",))


def split(x):
    hi = x.astype(BF16)
    return hi, (x - hi.astype(F32)).astype(BF16)


def apply_block(mcat, vec):
    blk = mcat.shape[0]
    hi, lo = split(vec)
    out = jnp.dot(mcat, jnp.concatenate([hi, hi], axis=0), preferred_element_type=F32)
    return out + jnp.dot(mcat[:, :blk], lo, preferred_element_type=F32)


def column(row, blk):
    r = lax.broadcasted_iota(jnp.int32, (blk, blk), 0)
    c = lax.broadcasted_iota(jnp.int32, (blk, blk), 1)
    return jnp.sum(jnp.where(r == c, jnp.broadcast_to(row, (blk, blk)), 0.0), axis=1, keepdims=True)


def colsum(x):
    return jnp.sum(x, axis=0, keepdims=True)


def on_device(schur, interface_diag, precond, load, face_blocks):
    nblk, blk = precond.shape[3], precond.shape[4]
    cols = load.shape[-1]
    order = nblk * blk
    cap = face_blocks.shape[-1]
    slots = 6 * cap
    rows = cap * blk
    table = face_blocks.reshape(6, cap).T
    matrix = schur.reshape(order, order)
    diag = interface_diag.reshape(nblk, blk)

    def entry(table_ref, k, d):
        if isinstance(d, int) and d < 4:
            return table_ref[k, d]
        kept = (lax.axis_index("gz_1") == 0) | (d < 4)
        return table_ref[k, jnp.where(kept, d, 9 - d)]

    def pick(table_ref, i):
        b = entry(table_ref, i % cap, i // cap)
        return jnp.minimum(b, nblk - 1), (b < nblk).astype(F32)

    def pack():
        def body(table_ref, load_ref, pre_ref, *outs):
            for i in range(slots):
                b, m = pick(table_ref, i)
                out, at = outs[i // cap], (i % cap) * blk
                out[at : at + blk, :cols] = load_ref[pl.ds(pl.multiple_of(b * blk, blk), blk), :].astype(F32) * m
                out[at : at + blk, cols:] = pre_ref[b] * m

        return call(
            body,
            [((rows, cols + blk), F32)] * 6,
            (
                table,
                pltpu.with_memory_space_constraint(load.reshape(order, cols), pltpu.HBM),
                pltpu.with_memory_space_constraint(precond.reshape(nblk, blk, blk), pltpu.HBM),
            ),
            flops=10**8,
            hbm_table=True,
        )

    faces = pack()
    came = [x for a in range(3) for x in exchange(faces[2 * a], faces[2 * a + 1], AXES[a])]

    def fetch(table_ref, matrix_ref, s_ref, row_buf, sems):
        copies = []
        for i in range(slots):
            b, _ = pick(table_ref, i)
            copy = pltpu.make_async_copy(
                matrix_ref.at[pl.ds(pl.multiple_of(b * blk, blk), blk), :],
                row_buf.at[pl.ds(i * blk, blk), :],
                sems.at[i],
            )
            copy.start()
            copies.append(copy)
        for i in range(slots):
            copies[i].wait()
            for j in range(slots):
                b, _ = pick(table_ref, j)
                s_ref[i * blk : (i + 1) * blk, j * blk : (j + 1) * blk] = row_buf[
                    i * blk : (i + 1) * blk, pl.ds(pl.multiple_of(b * blk, blk), blk)
                ]

    def live_part():
        return call(
            fetch,
            [((slots * blk, slots * blk), BF16)],
            (table, matrix),
            scratch=(pltpu.VMEM((slots * blk, order), BF16), pltpu.SemaphoreType.DMA((slots,))),
            raw=(1,),
            flops=2 * 10**9,
        )[0]

    sel = live_part()

    def local_schur(table_ref, d, s_ref, zb_ref, z_ref, diag_ref, out_ref):
        base = d * rows if isinstance(d, int) else pl.multiple_of(d * rows, rows)
        product = jnp.dot(s_ref[pl.ds(base, rows), :], zb_ref[...], preferred_element_type=F32)
        for k in range(cap):
            b = entry(table_ref, k, d)
            m = (b < nblk).astype(F32)
            dcol = column(diag_ref[pl.ds(jnp.minimum(b, nblk - 1), 1), :], blk)
            z = z_ref[pl.ds(base + k * blk, blk), :]
            out_ref[k * blk : (k + 1) * blk, :] = (product[k * blk : (k + 1) * blk] + dcol * z) * m

    long = slots * blk
    tall = (long, cols)
    flat = (rows, cols)

    def first(table_ref, *refs):
        own, got = refs[:6], refs[6:12]
        diag_ref, s_ref = refs[12:14]
        r_ref, z_ref, m_ref = refs[14:17]
        y_refs, zb_ref = refs[17:23], refs[23]
        for i in range(slots):
            d, at = i // cap, (i % cap) * blk
            r = own[d][at : at + blk, :cols] + got[d][at : at + blk, :cols]
            m = own[d][at : at + blk, cols:] + got[d][at : at + blk, cols:]
            hi, lo = split(m)
            mcat = jnp.concatenate([hi, lo], axis=1)
            m_ref[i * blk : (i + 1) * blk, :] = mcat
            r_ref[i * blk : (i + 1) * blk, :] = r
            z = apply_block(mcat, r)
            z_ref[i * blk : (i + 1) * blk, :] = z
            zb_ref[i * blk : (i + 1) * blk, :] = z.astype(BF16)
        for d in range(6):
            local_schur(table_ref, d, s_ref, zb_ref, z_ref, diag_ref, y_refs[d])

    r, z1, mcat, *ys = call(
        first,
        [(tall, F32), (tall, F32), ((long, 2 * blk), BF16)] + [(flat, F32)] * 6,
        (table, *faces, *came, diag, sel),
        scratch=(pltpu.VMEM(tall, BF16),),
        flops=2 * 10**9,
    )
    came = [x for a in range(3) for x in exchange(ys[2 * a], ys[2 * a + 1], AXES[a])]

    def sides(axis):
        low = lax.axis_index("gz_1") == 0
        return jnp.where(low, 2 * axis, 2 * axis + 1), jnp.where(low, 2 * axis + 1, 2 * axis)

    def second(table_ref, *refs, given=False):
        if given:
            raw_ref, r_ref, gram_ref = refs[:3]
            scale = 1.0 / jnp.sqrt(gram_ref[0:1, :] + epsilon)
            h11 = gram_ref[1:2, :] * scale * scale
            refs = refs[3:]
        else:
            own, got = refs[:6], refs[6:12]
            refs = refs[12:]
        m_ref, diag_ref, s_ref = refs[:3]
        w_ref, z_ref, zb_ref = refs[3:6]
        msg_refs = refs[6:9]
        for i in range(slots):
            d, at = i // cap, (i % cap) * blk
            if given:
                w = raw_ref[i * blk : (i + 1) * blk, :] - h11 * r_ref[i * blk : (i + 1) * blk, :]
                w = w * scale
                r = r_ref[i * blk : (i + 1) * blk, :]
                refs[9][i * blk : (i + 1) * blk, :] = apply_block(m_ref[i * blk : (i + 1) * blk, :], r)
            else:
                w = own[d][at : at + blk, :] + got[d][at : at + blk, :]
            w_ref[i * blk : (i + 1) * blk, :] = w
            z = apply_block(m_ref[i * blk : (i + 1) * blk, :], w)
            z_ref[i * blk : (i + 1) * blk, :] = z
            zb_ref[i * blk : (i + 1) * blk, :] = z.astype(BF16)
        for a in range(3):
            local_schur(table_ref, sides(a)[0], s_ref, zb_ref, z_ref, diag_ref, msg_refs[a])

    def rest_of_second(table_ref, zb_ref, z_ref, diag_ref, s_ref, *keep_refs):
        for a in range(3):
            local_schur(table_ref, sides(a)[1], s_ref, zb_ref, z_ref, diag_ref, keep_refs[a])

    def dots(*refs):
        y_refs, msg_refs, keep_refs = refs[:6], refs[6:9], refs[9:12]
        r_ref, w_ref, out_ref = refs[12:15]
        sums = [jnp.zeros((1, cols), F32) for _ in range(5)]
        for d in range(6):
            r = r_ref[d * rows : (d + 1) * rows, :]
            w = w_ref[d * rows : (d + 1) * rows, :]
            sums[0] += 0.5 * colsum(r * r)
            sums[1] += colsum(r * y_refs[d][...])
            sums[2] += 0.5 * colsum(w * w)
        for a in range(3):
            for d, ref in zip(sides(a), (msg_refs[a], keep_refs[a])):
                at = pl.ds(pl.multiple_of(d * rows, rows), rows)
                y = ref[...]
                sums[3] += colsum(y * r_ref[at, :])
                sums[4] += colsum(y * w_ref[at, :])
        out_ref[...] = jnp.zeros_like(out_ref)
        for i in range(5):
            out_ref[i : i + 1, :] = sums[i]

    def norms(*refs):
        keep_refs, got, in_ref, out_ref = refs[:3], refs[3:6], refs[6], refs[7]
        out_ref[...] = in_ref[...]
        square = jnp.zeros((1, cols), F32)
        for a in range(3):
            both = keep_refs[a][...] + got[a][...]
            square += colsum(both * both)
        out_ref[5:6, :] = square

    def second_step(ys, heads, mcat, sel, r, given=False):
        w, z, zb, *rest = call(
            functools.partial(second, given=given),
            [(tall, F32), (tall, F32), (tall, BF16)] + [(flat, F32)] * 3 + [(tall, F32)] * given,
            (table, *heads, mcat, diag, sel),
            flops=2 * 10**9,
        )
        msgs, z1 = rest[:3], rest[3:]
        got = []
        for a in range(3):
            got.append(exchange_once(msgs[a], AXES[a]))
        keeps = call(
            rest_of_second, [(flat, F32)] * 3, (table, zb, z, diag, sel), flops=10**9
        )
        (sums,) = call(dots, [((8, cols), F32)], (*ys, *msgs, *keeps, r, w), smem=0, flops=10**9)
        (sums,) = call(norms, [((8, cols), F32)], (*keeps, *got, sums), smem=0)
        return w, z, total(sums), z1

    w1, z2, sums, _ = second_step(ys, (*ys, *came), mcat, sel, r)

    def weights(initial, h11, h21, h12, h22, h32):
        r1 = jnp.sqrt(h11 * h11 + h21 * h21)
        c1, s1 = h11 / r1, h21 / r1
        top = c1 * h12 + s1 * h22
        bottom = c1 * h22 - s1 * h12
        r2 = jnp.sqrt(bottom * bottom + h32 * h32)
        c2, s2 = bottom / r2, h32 / r2
        y2 = -initial * s1 * c2 / r2
        y1 = (initial * c1 - top * y2) / r1
        return y1, y2, initial * s1 * s2

    def gram_rest(square, h12, dot22, g11, g12, g22):
        h22 = dot22 - h12 * g12
        left = square - h12 * h12 * (2.0 - g11) - h22 * (2.0 * dot22 - h22 * g22)
        return h22, left + 2.0 * h12 * h22 * g12

    def store(table_ref, z1_ref, z2_ref, a1, a2, out_ref):
        out_ref[...] = jnp.zeros_like(out_ref)
        for i in range(slots):
            b = entry(table_ref, i % cap, i // cap)

            @pl.when(b < nblk)
            def _():
                z = a1 * z1_ref[i * blk : (i + 1) * blk, :] + a2 * z2_ref[i * blk : (i + 1) * blk, :]
                out_ref[pl.ds(pl.multiple_of(b * blk, blk), blk), :] = z

    def finish(table_ref, z1_ref, z2_ref, gram_ref, out_ref, res_ref, flag_ref, slot_ref, buf_ref, sems):
        for b in range(nblk):
            slot_ref[b] = jnp.int32(-1)
        for i in range(slots):
            slot_ref[entry(table_ref, i % cap, i // cap)] = jnp.int32(i)
        load_square = gram_ref[0:1, :]
        initial = jnp.sqrt(load_square + epsilon)
        rescale = 1.0 / initial
        scale2 = rescale * rescale
        h11 = gram_ref[1:2, :] * scale2
        b11 = gram_ref[2:3, :] * scale2
        c1v = gram_ref[3:4, :] * scale2
        c11 = gram_ref[4:5, :] * scale2
        e11 = gram_ref[5:6, :] * scale2
        g11 = load_square * scale2
        w_square = jnp.maximum(b11 - h11 * h11 * (2.0 - g11), 0.0)
        h21 = jnp.sqrt(w_square + epsilon)
        down = 1.0 / h21
        g22 = w_square * down * down
        g12 = h11 * (epsilon * scale2) * down
        h12 = (c1v - h11 * h11) * down
        dot22 = ((c11 - h11 * c1v) - h11 * (b11 - h11 * h11)) * down * down
        square = ((e11 - h11 * c11) - h11 * (c11 - h11 * b11)) * down * down
        h22, left = gram_rest(square, h12, dot22, g11, g12, g22)
        h32 = jnp.sqrt(jnp.maximum(left, 0.0) + epsilon)
        y1, y2, res = weights(initial, h11, h21, h12, h22, h32)
        a2 = y2 * down * rescale
        res_ref[...] = res
        a1 = y1 * rescale - a2 * h11
        copies = []
        for g in range(STEPS):
            for b in range(g * nblk // STEPS, (g + 1) * nblk // STEPS):
                slot = slot_ref[b]
                m = (slot >= 0).astype(F32)
                at = pl.ds(pl.multiple_of(jnp.maximum(slot, 0) * blk, blk), blk)
                z = (a1 * m) * z1_ref[at, :] + (a2 * m) * z2_ref[at, :]
                buf_ref[b * blk : (b + 1) * blk, :] = z
            part = pl.ds(g * (order // STEPS), order // STEPS)
            copies.append(pltpu.make_async_copy(buf_ref.at[part, :], out_ref.at[part, :], sems.at[g]))
            copies[-1].start()
        kept = (w_square >= TRUST * b11) & (left * (w_square + epsilon) >= TRUST * e11)
        flag_ref[0] = 1 - jnp.min(kept.astype(F32)).astype(jnp.int32)
        for copy in copies:
            copy.wait()

    def finish_again(table_ref, z1_ref, z2_ref, one_ref, two_ref, out_ref, res_ref):
        load_square = one_ref[0:1, :]
        initial = jnp.sqrt(load_square + epsilon)
        rescale = 1.0 / initial
        h11 = one_ref[1:2, :] * rescale * rescale
        w_square = two_ref[2:3, :]
        h21 = jnp.sqrt(w_square + epsilon)
        down = 1.0 / h21
        g11 = load_square * rescale * rescale
        g22 = w_square * down * down
        g12 = h11 * (epsilon * rescale * rescale) * down
        h12 = two_ref[3:4, :] * rescale * down
        dot22 = two_ref[4:5, :] * down * down
        square = two_ref[5:6, :] * down * down
        h22, left = gram_rest(square, h12, dot22, g11, g12, g22)
        h32 = jnp.sqrt(jnp.maximum(left, 0.0) + epsilon)
        y1, y2, res = weights(initial, h11, h21, h12, h22, h32)
        res_ref[...] = res
        store(table_ref, z1_ref, z2_ref, y1 * rescale, y2 * down, out_ref)

    results = [((order, cols), F32), ((1, cols), F32)]
    out, res, flag = pl.pallas_call(
        finish,
        out_shape=[jax.ShapeDtypeStruct(shape, t) for shape, t in results]
        + [jax.ShapeDtypeStruct((1,), jnp.int32)],
        in_specs=[pl.BlockSpec(memory_space=pltpu.SMEM)] + [pl.BlockSpec(memory_space=pltpu.VMEM)] * 3,
        out_specs=[
            pl.BlockSpec(memory_space=pltpu.HBM),
            pl.BlockSpec(memory_space=pltpu.VMEM),
            pl.BlockSpec(memory_space=pltpu.SMEM),
        ],
        scratch_shapes=[
            pltpu.SMEM((nblk + 1,), jnp.int32),
            pltpu.VMEM((order, cols), F32),
            pltpu.SemaphoreType.DMA((STEPS,)),
        ],
        compiler_params=pltpu.CompilerParams(vmem_limit_bytes=16 * 2**20),
    )(table, z1, z2, sums)

    def careful(state):
        r, w1, mcat = (pltpu.with_memory_space_constraint(x, pltpu.HBM) for x in state[3:6])
        sums = state[6]
        zeros = [jnp.zeros(flat, F32)] * 6
        _, z2, more, (z1,) = second_step(zeros, (w1, r, sums), mcat, live_part(), r, given=True)
        out, res = call(finish_again, results, (table, z1, z2, sums, more))
        return jnp.zeros((1,), jnp.int32), out, res, *state[3:]

    _, out, res, *_ = lax.while_loop(
        lambda state: state[0][0] > 0, careful, (flag, out, res, r, w1, mcat, sums)
    )
    return out.reshape(1, 1, 1, order, cols), res.reshape(cols)


def solution(mesh):
    torus = Mesh(
        mesh.devices.reshape(mesh.shape["gx"], mesh.shape["gy"], 4, 2), ("gx", "gy", "gz_0", "gz_1")
    )
    in_specs = (
        P("gx", "gy", GZ, None, None),
        P("gx", "gy", GZ, None),
        P("gx", "gy", GZ, None, None, None),
        P("gx", "gy", GZ, None, None),
        P("gx", "gy", GZ, None, None),
    )
    out_specs = (P("gx", "gy", GZ, None, None), P())
    return jax.shard_map(
        on_device, mesh=torus, in_specs=in_specs, out_specs=out_specs, check_vma=False
    )
```

```python
import functools

import jax
import jax.numpy as jnp
from jax import lax
from jax.experimental import pallas as pl
from jax.experimental.pallas import tpu as pltpu
from jax.sharding import Mesh
from jax.sharding import PartitionSpec as P

GZ = ("gz_0", "gz_1")
STEPS = 4
AXES = ("gx", "gy", GZ)
INNER = ("gy", "gz_0", "gz_1")


epsilon = 1e-06
TRUST = 1e-3
F32 = jnp.float32
BF16 = jnp.bfloat16


def call(body, outs, operands, scratch=(), smem=1, raw=(), flops=0, mib=16, hbm_table=False):
    specs = []
    operands = list(operands)
    for i in range(len(operands)):
        if i < smem:
            specs.append(pl.BlockSpec(memory_space=pltpu.SMEM))
            if hbm_table:
                operands[i] = pltpu.with_memory_space_constraint(operands[i], pltpu.HBM)
        elif i in raw:
            specs.append(pl.BlockSpec(memory_space=pltpu.HBM))
            operands[i] = pltpu.with_memory_space_constraint(operands[i], pltpu.HBM)
        else:
            specs.append(pl.BlockSpec(memory_space=pltpu.VMEM))
    return pl.pallas_call(
        body,
        out_shape=[jax.ShapeDtypeStruct(s, t) for s, t in outs],
        in_specs=specs,
        out_specs=[pl.BlockSpec(memory_space=pltpu.VMEM) for _ in outs],
        scratch_shapes=list(scratch),
        compiler_params=pltpu.CompilerParams(vmem_limit_bytes=mib * 2**20),
        cost_estimate=pl.CostEstimate(flops=flops, transcendentals=0, bytes_accessed=2**20),
    )(*operands)


def shifts(axis):
    n = lax.axis_size(axis)
    up = [(i, (i + 1) % n) for i in range(n)]
    return up, [(j, i) for i, j in up]


def exchange(first, second, axis):
    n = lax.axis_size(axis)
    return [
        lax.ppermute(first, axis, [(i, i ^ 1) for i in range(n)]),
        lax.ppermute(second, axis, [(i, (i - 1 + 2 * (i % 2)) % n) for i in range(n)]),
    ]


def even(axis):
    return lax.axis_index(("gx", "gy", "gz_1")[axis]) % 2 == 0


def exchange_once(message, axis):
    if axis == GZ:
        return lax.ppermute(message, GZ, shifts(GZ)[0])
    n = lax.axis_size(axis)
    pairs = []
    for i in range(n):
        pairs += [(2 * i, 2 * ((i + 1) % n)), (2 * i + 1, 2 * ((i - 1) % n) + 1)]
    return lax.ppermute(message, (axis, "gz_1"), pairs)


def gather_sum(rows, axes):
    n = lax.axis_size(axes)
    wide = jnp.broadcast_to(rows[None], (n,) + rows.shape).reshape(n * rows.shape[0], rows.shape[1])
    wide = lax.all_to_all(wide, axes, 0, 0, tiled=True)
    return jnp.sum(wide.reshape((n,) + rows.shape), axis=0)


def total(rows):
    return gather_sum(gather_sum(rows, INNER), ("gx",))


def split(x):
    hi = x.astype(BF16)
    return hi, (x - hi.astype(F32)).astype(BF16)


def apply_block(mcat, vec):
    blk = mcat.shape[0]
    hi, lo = split(vec)
    out = jnp.dot(mcat, jnp.concatenate([hi, hi], axis=0), preferred_element_type=F32)
    return out + jnp.dot(mcat[:, :blk], lo, preferred_element_type=F32)


def column(row, blk):
    r = lax.broadcasted_iota(jnp.int32, (blk, blk), 0)
    c = lax.broadcasted_iota(jnp.int32, (blk, blk), 1)
    return jnp.sum(jnp.where(r == c, jnp.broadcast_to(row, (blk, blk)), 0.0), axis=1, keepdims=True)


def colsum(x):
    return jnp.sum(x, axis=0, keepdims=True)


def on_device(schur, interface_diag, precond, load, face_blocks):
    nblk, blk = precond.shape[3], precond.shape[4]
    cols = load.shape[-1]
    order = nblk * blk
    cap = face_blocks.shape[-1]
    slots = 6 * cap
    rows = cap * blk
    table = face_blocks.reshape(6, cap).T
    matrix = schur.reshape(order, order)
    diag = interface_diag.reshape(nblk, blk)

    def entry(table_ref, k, d):
        if isinstance(d, int):
            return table_ref[k, jnp.where(even(d // 2), d, d ^ 1)]
        flips = [jnp.where(even(a), 0, 1) for a in range(3)]
        flip = jnp.where(d < 2, flips[0], jnp.where(d < 4, flips[1], flips[2]))
        return table_ref[k, d + flip * (1 - 2 * (d % 2))]

    def pick(table_ref, i):
        b = entry(table_ref, i % cap, i // cap)
        return jnp.minimum(b, nblk - 1), (b < nblk).astype(F32)

    def pack():
        def body(table_ref, load_ref, pre_ref, *outs):
            for i in range(slots):
                b, m = pick(table_ref, i)
                out, at = outs[i // cap], (i % cap) * blk
                out[at : at + blk, :cols] = load_ref[pl.ds(pl.multiple_of(b * blk, blk), blk), :].astype(F32) * m
                out[at : at + blk, cols:] = pre_ref[b] * m

        return call(
            body,
            [((rows, cols + blk), F32)] * 6,
            (
                table,
                pltpu.with_memory_space_constraint(load.reshape(order, cols), pltpu.HBM),
                pltpu.with_memory_space_constraint(precond.reshape(nblk, blk, blk), pltpu.HBM),
            ),
            flops=10**8,
            hbm_table=True,
        )

    faces = pack()
    came = [x for a in range(3) for x in exchange(faces[2 * a], faces[2 * a + 1], AXES[a])]

    def fetch(table_ref, matrix_ref, s_ref, row_buf, sems):
        copies = []
        for i in range(slots):
            b, _ = pick(table_ref, i)
            copy = pltpu.make_async_copy(
                matrix_ref.at[pl.ds(pl.multiple_of(b * blk, blk), blk), :],
                row_buf.at[pl.ds(i * blk, blk), :],
                sems.at[i],
            )
            copy.start()
            copies.append(copy)
        for i in range(slots):
            copies[i].wait()
            for j in range(slots):
                b, _ = pick(table_ref, j)
                s_ref[i * blk : (i + 1) * blk, j * blk : (j + 1) * blk] = row_buf[
                    i * blk : (i + 1) * blk, pl.ds(pl.multiple_of(b * blk, blk), blk)
                ]

    def live_part():
        return call(
            fetch,
            [((slots * blk, slots * blk), BF16)],
            (table, matrix),
            scratch=(pltpu.VMEM((slots * blk, order), BF16), pltpu.SemaphoreType.DMA((slots,))),
            raw=(1,),
            flops=2 * 10**9,
        )[0]

    sel = live_part()

    def local_schur(table_ref, d, s_ref, zb_ref, z_ref, diag_ref, out_ref):
        base = d * rows if isinstance(d, int) else pl.multiple_of(d * rows, rows)
        product = jnp.dot(s_ref[pl.ds(base, rows), :], zb_ref[...], preferred_element_type=F32)
        for k in range(cap):
            b = entry(table_ref, k, d)
            m = (b < nblk).astype(F32)
            dcol = column(diag_ref[pl.ds(jnp.minimum(b, nblk - 1), 1), :], blk)
            z = z_ref[pl.ds(base + k * blk, blk), :]
            out_ref[k * blk : (k + 1) * blk, :] = (product[k * blk : (k + 1) * blk] + dcol * z) * m

    long = slots * blk
    tall = (long, cols)
    flat = (rows, cols)

    def first(table_ref, *refs):
        own, got = refs[:6], refs[6:12]
        diag_ref, s_ref = refs[12:14]
        r_ref, z_ref, m_ref = refs[14:17]
        y_refs, zb_ref = refs[17:23], refs[23]
        for i in range(slots):
            d, at = i // cap, (i % cap) * blk
            r = own[d][at : at + blk, :cols] + got[d][at : at + blk, :cols]
            m = own[d][at : at + blk, cols:] + got[d][at : at + blk, cols:]
            hi, lo = split(m)
            mcat = jnp.concatenate([hi, lo], axis=1)
            m_ref[i * blk : (i + 1) * blk, :] = mcat
            r_ref[i * blk : (i + 1) * blk, :] = r
            z = apply_block(mcat, r)
            z_ref[i * blk : (i + 1) * blk, :] = z
            zb_ref[i * blk : (i + 1) * blk, :] = z.astype(BF16)
        for d in range(6):
            local_schur(table_ref, d, s_ref, zb_ref, z_ref, diag_ref, y_refs[d])

    r, z1, mcat, *ys = call(
        first,
        [(tall, F32), (tall, F32), ((long, 2 * blk), BF16)] + [(flat, F32)] * 6,
        (table, *faces, *came, diag, sel),
        scratch=(pltpu.VMEM(tall, BF16),),
        flops=2 * 10**9,
    )
    came = [x for a in range(3) for x in exchange(ys[2 * a], ys[2 * a + 1], AXES[a])]

    def sides(axis):
        up = lax.axis_index("gz_1") == 0
        partner = even(axis) == up if axis < 2 else up
        return jnp.where(partner, 2 * axis, 2 * axis + 1), jnp.where(partner, 2 * axis + 1, 2 * axis)

    def second(table_ref, *refs, given=False):
        if given:
            raw_ref, r_ref, gram_ref = refs[:3]
            scale = 1.0 / jnp.sqrt(gram_ref[0:1, :] + epsilon)
            h11 = gram_ref[1:2, :] * scale * scale
            refs = refs[3:]
        else:
            own, got = refs[:6], refs[6:12]
            refs = refs[12:]
        m_ref, diag_ref, s_ref = refs[:3]
        w_ref, z_ref, zb_ref = refs[3:6]
        msg_refs = refs[6:9]
        for i in range(slots):
            d, at = i // cap, (i % cap) * blk
            if given:
                w = raw_ref[i * blk : (i + 1) * blk, :] - h11 * r_ref[i * blk : (i + 1) * blk, :]
                w = w * scale
                r = r_ref[i * blk : (i + 1) * blk, :]
                refs[9][i * blk : (i + 1) * blk, :] = apply_block(m_ref[i * blk : (i + 1) * blk, :], r)
            else:
                w = own[d][at : at + blk, :] + got[d][at : at + blk, :]
            w_ref[i * blk : (i + 1) * blk, :] = w
            z = apply_block(m_ref[i * blk : (i + 1) * blk, :], w)
            z_ref[i * blk : (i + 1) * blk, :] = z
            zb_ref[i * blk : (i + 1) * blk, :] = z.astype(BF16)
        for a in range(3):
            local_schur(table_ref, sides(a)[0], s_ref, zb_ref, z_ref, diag_ref, msg_refs[a])

    def rest_of_second(table_ref, zb_ref, z_ref, diag_ref, s_ref, *keep_refs):
        for a in range(3):
            local_schur(table_ref, sides(a)[1], s_ref, zb_ref, z_ref, diag_ref, keep_refs[a])

    def dots(*refs):
        y_refs, msg_refs, keep_refs = refs[:6], refs[6:9], refs[9:12]
        r_ref, w_ref, out_ref = refs[12:15]
        sums = [jnp.zeros((1, cols), F32) for _ in range(5)]
        for d in range(6):
            r = r_ref[d * rows : (d + 1) * rows, :]
            w = w_ref[d * rows : (d + 1) * rows, :]
            sums[0] += 0.5 * colsum(r * r)
            sums[1] += colsum(r * y_refs[d][...])
            sums[2] += 0.5 * colsum(w * w)
        for a in range(3):
            for d, ref in zip(sides(a), (msg_refs[a], keep_refs[a])):
                at = pl.ds(pl.multiple_of(d * rows, rows), rows)
                y = ref[...]
                sums[3] += colsum(y * r_ref[at, :])
                sums[4] += colsum(y * w_ref[at, :])
        out_ref[...] = jnp.zeros_like(out_ref)
        for i in range(5):
            out_ref[i : i + 1, :] = sums[i]

    def norms(*refs):
        keep_refs, got, in_ref, out_ref = refs[:3], refs[3:6], refs[6], refs[7]
        out_ref[...] = in_ref[...]
        square = jnp.zeros((1, cols), F32)
        for a in range(3):
            both = keep_refs[a][...] + got[a][...]
            square += colsum(both * both)
        out_ref[5:6, :] = square

    def second_step(ys, heads, mcat, sel, r, given=False):
        w, z, zb, *rest = call(
            functools.partial(second, given=given),
            [(tall, F32), (tall, F32), (tall, BF16)] + [(flat, F32)] * 3 + [(tall, F32)] * given,
            (table, *heads, mcat, diag, sel),
            flops=2 * 10**9,
        )
        msgs, z1 = rest[:3], rest[3:]
        got = []
        for a in range(3):
            got.append(exchange_once(msgs[a], AXES[a]))
        keeps = call(
            rest_of_second, [(flat, F32)] * 3, (table, zb, z, diag, sel), flops=10**9
        )
        (sums,) = call(dots, [((8, cols), F32)], (*ys, *msgs, *keeps, r, w), smem=0, flops=10**9)
        (sums,) = call(norms, [((8, cols), F32)], (*keeps, *got, sums), smem=0)
        return w, z, total(sums), z1

    w1, z2, sums, _ = second_step(ys, (*ys, *came), mcat, sel, r)

    def weights(initial, h11, h21, h12, h22, h32):
        r1 = jnp.sqrt(h11 * h11 + h21 * h21)
        c1, s1 = h11 / r1, h21 / r1
        top = c1 * h12 + s1 * h22
        bottom = c1 * h22 - s1 * h12
        r2 = jnp.sqrt(bottom * bottom + h32 * h32)
        c2, s2 = bottom / r2, h32 / r2
        y2 = -initial * s1 * c2 / r2
        y1 = (initial * c1 - top * y2) / r1
        return y1, y2, initial * s1 * s2

    def gram_rest(square, h12, dot22, g11, g12, g22):
        h22 = dot22 - h12 * g12
        left = square - h12 * h12 * (2.0 - g11) - h22 * (2.0 * dot22 - h22 * g22)
        return h22, left + 2.0 * h12 * h22 * g12

    def store(table_ref, z1_ref, z2_ref, a1, a2, out_ref):
        out_ref[...] = jnp.zeros_like(out_ref)
        for i in range(slots):
            b = entry(table_ref, i % cap, i // cap)

            @pl.when(b < nblk)
            def _():
                z = a1 * z1_ref[i * blk : (i + 1) * blk, :] + a2 * z2_ref[i * blk : (i + 1) * blk, :]
                out_ref[pl.ds(pl.multiple_of(b * blk, blk), blk), :] = z

    def finish(table_ref, z1_ref, z2_ref, gram_ref, out_ref, res_ref, flag_ref, slot_ref, buf_ref, sems):
        for b in range(nblk):
            slot_ref[b] = jnp.int32(-1)
        for i in range(slots):
            slot_ref[entry(table_ref, i % cap, i // cap)] = jnp.int32(i)
        load_square = gram_ref[0:1, :]
        initial = jnp.sqrt(load_square + epsilon)
        rescale = 1.0 / initial
        scale2 = rescale * rescale
        h11 = gram_ref[1:2, :] * scale2
        b11 = gram_ref[2:3, :] * scale2
        c1v = gram_ref[3:4, :] * scale2
        c11 = gram_ref[4:5, :] * scale2
        e11 = gram_ref[5:6, :] * scale2
        g11 = load_square * scale2
        w_square = jnp.maximum(b11 - h11 * h11 * (2.0 - g11), 0.0)
        h21 = jnp.sqrt(w_square + epsilon)
        down = 1.0 / h21
        g22 = w_square * down * down
        g12 = h11 * (epsilon * scale2) * down
        h12 = (c1v - h11 * h11) * down
        dot22 = ((c11 - h11 * c1v) - h11 * (b11 - h11 * h11)) * down * down
        square = ((e11 - h11 * c11) - h11 * (c11 - h11 * b11)) * down * down
        h22, left = gram_rest(square, h12, dot22, g11, g12, g22)
        h32 = jnp.sqrt(jnp.maximum(left, 0.0) + epsilon)
        y1, y2, res = weights(initial, h11, h21, h12, h22, h32)
        a2 = y2 * down * rescale
        res_ref[...] = res
        a1 = y1 * rescale - a2 * h11
        copies = []
        for g in range(STEPS):
            for b in range(g * nblk // STEPS, (g + 1) * nblk // STEPS):
                slot = slot_ref[b]
                m = (slot >= 0).astype(F32)
                at = pl.ds(pl.multiple_of(jnp.maximum(slot, 0) * blk, blk), blk)
                z = (a1 * m) * z1_ref[at, :] + (a2 * m) * z2_ref[at, :]
                buf_ref[b * blk : (b + 1) * blk, :] = z
            part = pl.ds(g * (order // STEPS), order // STEPS)
            copies.append(pltpu.make_async_copy(buf_ref.at[part, :], out_ref.at[part, :], sems.at[g]))
            copies[-1].start()
        kept = (w_square >= TRUST * b11) & (left * (w_square + epsilon) >= TRUST * e11)
        flag_ref[0] = 1 - jnp.min(kept.astype(F32)).astype(jnp.int32)
        for copy in copies:
            copy.wait()

    def finish_again(table_ref, z1_ref, z2_ref, one_ref, two_ref, out_ref, res_ref):
        load_square = one_ref[0:1, :]
        initial = jnp.sqrt(load_square + epsilon)
        rescale = 1.0 / initial
        h11 = one_ref[1:2, :] * rescale * rescale
        w_square = two_ref[2:3, :]
        h21 = jnp.sqrt(w_square + epsilon)
        down = 1.0 / h21
        g11 = load_square * rescale * rescale
        g22 = w_square * down * down
        g12 = h11 * (epsilon * rescale * rescale) * down
        h12 = two_ref[3:4, :] * rescale * down
        dot22 = two_ref[4:5, :] * down * down
        square = two_ref[5:6, :] * down * down
        h22, left = gram_rest(square, h12, dot22, g11, g12, g22)
        h32 = jnp.sqrt(jnp.maximum(left, 0.0) + epsilon)
        y1, y2, res = weights(initial, h11, h21, h12, h22, h32)
        res_ref[...] = res
        store(table_ref, z1_ref, z2_ref, y1 * rescale, y2 * down, out_ref)

    results = [((order, cols), F32), ((1, cols), F32)]
    out, res, flag = pl.pallas_call(
        finish,
        out_shape=[jax.ShapeDtypeStruct(shape, t) for shape, t in results]
        + [jax.ShapeDtypeStruct((1,), jnp.int32)],
        in_specs=[pl.BlockSpec(memory_space=pltpu.SMEM)] + [pl.BlockSpec(memory_space=pltpu.VMEM)] * 3,
        out_specs=[
            pl.BlockSpec(memory_space=pltpu.HBM),
            pl.BlockSpec(memory_space=pltpu.VMEM),
            pl.BlockSpec(memory_space=pltpu.SMEM),
        ],
        scratch_shapes=[
            pltpu.SMEM((nblk + 1,), jnp.int32),
            pltpu.VMEM((order, cols), F32),
            pltpu.SemaphoreType.DMA((STEPS,)),
        ],
        compiler_params=pltpu.CompilerParams(vmem_limit_bytes=16 * 2**20),
    )(table, z1, z2, sums)

    def careful(state):
        r, w1, mcat = (pltpu.with_memory_space_constraint(x, pltpu.HBM) for x in state[3:6])
        sums = state[6]
        zeros = [jnp.zeros(flat, F32)] * 6
        _, z2, more, (z1,) = second_step(zeros, (w1, r, sums), mcat, live_part(), r, given=True)
        out, res = call(finish_again, results, (table, z1, z2, sums, more))
        return jnp.zeros((1,), jnp.int32), out, res, *state[3:]

    _, out, res, *_ = lax.while_loop(
        lambda state: state[0][0] > 0, careful, (flag, out, res, r, w1, mcat, sums)
    )
    return out.reshape(1, 1, 1, order, cols), res.reshape(cols)


def solution(mesh):
    torus = Mesh(
        mesh.devices.reshape(mesh.shape["gx"], mesh.shape["gy"], 4, 2), ("gx", "gy", "gz_0", "gz_1")
    )
    in_specs = (
        P("gx", "gy", GZ, None, None),
        P("gx", "gy", GZ, None),
        P("gx", "gy", GZ, None, None, None),
        P("gx", "gy", GZ, None, None),
        P("gx", "gy", GZ, None, None),
    )
    out_specs = (P("gx", "gy", GZ, None, None), P())
    return jax.shard_map(
        on_device, mesh=torus, in_specs=in_specs, out_specs=out_specs, check_vma=False
    )
```
